32 devices in a mesh: date: 4 (over y, x), pix: 8 (over z, core).
Axes of the slice: x: 2, y: 2, z: 4, core: 2. Of those that a mesh axis runs over, the one named last changes fastest.
Arguments:
- stack: bfloat16 [64, 7, 64, 1024], P('date', None, None, 'pix'), may hold values from -8 to 8
- quality: int32 [64, 64, 1024], P('date', None, 'pix'), may hold values from 0 to 1073741823
- days: int32 [64], P('date'), may hold values from 8 to 1536, as said below
Outputs:
- coef: float32 [7, 8, 64, 1024], P(None, None, 'pix', 'date')
- score: float32 [7, 64, 1024], P(None, 'pix', 'date')
The draws below stay inside these ranges and needn't reach their ends.
Inputs may be any that keep to these rules, and one draw needn't show every extreme that they name: `days`: strictly increasing.
All inputs are finite; a program needn't handle non-finite values.
Results may differ from the reference program's by a relative error of at most 0.0003.
Values may be sent and summed in bfloat16 or wider, within the bound.
A program may use at most 256 MiB of HBM per device.

```python
import jax
import jax.numpy as jnp
from jax import lax

DATES = 64
BANDS = 7
HARM = 8
ROWS = 64
COLS = 1024


def make_days(key):
    inner_count = 24 * DATES - 9
    order = jax.random.permutation(jax.random.fold_in(key, 11), inner_count)
    chosen = jnp.sort(order[:DATES - 2]).astype(jnp.int32) + 9
    first = jnp.full((1,), 8, dtype=jnp.int32)
    last = jnp.full((1,), 24 * DATES, dtype=jnp.int32)
    return jnp.concatenate([first, chosen, last]).astype(jnp.int32)


def design_matrix_drawn(days):
    moment_t = days.astype(jnp.float32)
    columns = [jnp.ones_like(moment_t), (moment_t - 512.0) / 512.0]
    for order in range(1, 4):
        phase = 2.0 * jnp.pi * order * moment_t / 365.25
        columns.append(jnp.cos(phase))
        columns.append(jnp.sin(phase))
    return jnp.stack(columns, 1)


def draw_days(key, part):
    return make_days(key)


def draw_quality(key, part):
    shape = (DATES, ROWS, COLS)
    bits = jax.random.randint(jax.random.fold_in(key, 21), shape, 0, 2 ** 30)
    rows = jnp.arange(ROWS, dtype=jnp.int32)
    cols = jnp.arange(COLS, dtype=jnp.int32)
    row_limit = 300 * rows // max(ROWS - 1, 1)
    col_limit = 300 * cols // max(COLS - 1, 1)
    limit = 200 + row_limit[:, None] + col_limit[None, :]
    rolled = jax.random.randint(jax.random.fold_in(key, 22), shape, 0, 1000)
    cloud = (rolled < limit[None, :, :]).astype(jnp.int32)
    return (bits - jnp.bitwise_and(bits, 8) + 8 * cloud).astype(jnp.int32)


def draw_stack(key, part):
    design = design_matrix_drawn(make_days(key))
    coefs = 0.6 * jax.random.normal(jax.random.fold_in(key, 31), (HARM, BANDS, ROWS, COLS), jnp.float32)
    rough = jax.random.uniform(jax.random.fold_in(key, 32), (BANDS, ROWS, COLS), jnp.float32, 0.5, 1.5)
    rows = jnp.arange(ROWS, dtype=jnp.float32)
    cols = jnp.arange(COLS, dtype=jnp.float32)
    row_scale = 0.15 * jnp.power(3.2, rows / max(ROWS - 1, 1))
    col_scale = jnp.power(3.2, cols / max(COLS - 1, 1))
    scale_map = row_scale[:, None] * col_scale[None, :]
    shape = (DATES, BANDS, ROWS, COLS)
    noise = jax.random.normal(jax.random.fold_in(key, 33), shape, jnp.float32)
    signal = jnp.einsum('tk,kbrc->tbrc', design, coefs)
    values = signal + noise * rough[None] * scale_map[None, None, :, :]
    return jnp.clip(values, -8.0, 8.0).astype(jnp.bfloat16)


def setup_inputs(seed: int = 0) -> dict:
    key_of = jax.random.split(jax.random.key(seed), 4)
    stack = draw_stack(jax.random.fold_in(key_of[3], 71), 0)
    quality = draw_quality(jax.random.fold_in(key_of[3], 71), 0)
    days = draw_days(jax.random.fold_in(key_of[3], 71), 0)
    return {"stack": stack, "quality": quality, "days": days}


RIDGE_TERM = 1.0
PAIR_LIST = [(first, second) for first in range(8) for second in range(first, 8)]

def design_matrix(days):
    moment_t = days.astype(jnp.float32)
    columns = [jnp.ones_like(moment_t), (moment_t - 512.0) / 512.0]
    for order in range(1, 4):
        phase = 2.0 * jnp.pi * order * moment_t / 365.25
        columns.append(jnp.cos(phase))
        columns.append(jnp.sin(phase))
    return jnp.stack(columns, 1)

def weights(quality):
    cloud = jnp.bitwise_and(jnp.right_shift(quality, 3), 1)
    level = jnp.bitwise_and(jnp.right_shift(quality, 8), 3)
    return (1 - cloud).astype(jnp.float32) / (1.0 + level.astype(jnp.float32))

def reference(stack, quality, days):
    design = design_matrix(days)
    products = jnp.stack([design[:, first] * design[:, second] for first, second in PAIR_LIST], 1)
    index_table = [[0] * 8 for first in range(8)]
    for number, pair in enumerate(PAIR_LIST):
        index_table[pair[0]][pair[1]] = number
        index_table[pair[1]][pair[0]] = number
    index_array = jnp.array(index_table, dtype=jnp.int32)
    high = lax.Precision.HIGHEST

    def row_fit(row):
        values = lax.dynamic_slice_in_dim(stack, row, 1, 2)[:, :, 0, :].astype(jnp.float32)
        bits = lax.dynamic_slice_in_dim(quality, row, 1, 1)[:, 0, :]
        weight = weights(bits)
        gram = jnp.dot(products.T, weight, precision=high)
        moment = jnp.einsum('tk,tbc->kbc', design, weight[:, None, :] * values, precision=high)
        full = jnp.transpose(gram[index_array], (2, 0, 1)) + RIDGE_TERM * jnp.eye(8, dtype=jnp.float32)
        solved = jnp.linalg.solve(full, jnp.transpose(moment, (2, 0, 1)))
        coef_row = jnp.transpose(solved, (1, 2, 0))
        fitted = jnp.einsum('tk,kbc->tbc', design, coef_row, precision=high)
        ssr = lax.optimization_barrier(jnp.sum(weight[:, None, :] * (values - fitted) ** 2, 0))
        return (coef_row, ssr, lax.optimization_barrier(jnp.sum(weight, 0)))
    coef_rows, ssr, wsum = lax.map(row_fit, jnp.arange(ROWS, dtype=jnp.int32))
    sigma2 = lax.optimization_barrier(jnp.sum(ssr, (0, 2))) / jnp.sum(wsum)
    score = jnp.sqrt(ssr / (wsum[:, None, :] + 1.0)) / jnp.sqrt(sigma2)[None, :, None]
    return (jnp.transpose(coef_rows, (2, 1, 0, 3)), jnp.transpose(score, (1, 0, 2)))
```

```python
import functools

import jax
import jax.numpy as jnp
from jax import lax
from jax.experimental import pallas as pl
from jax.experimental.pallas import tpu as pltpu
from jax.sharding import PartitionSpec as P

RIDGE_TERM = 1.0
HARM = 8
PAIR = 2
LAG = 2
LIMIT = 32767.0
LEVELS = 0x346C

MESH = pl.DeviceIdType.MESH
PAIR_LIST = [(first, second) for first in range(HARM) for second in range(first + 1)]
PAIR_AT = {pair: number for number, pair in enumerate(PAIR_LIST)}


def design_lanes(days):
    rows = [jnp.full((1, 128), day, jnp.int32) for day in days]
    moment_t = jnp.concatenate(rows, 0).astype(jnp.float32)
    lane = lax.broadcasted_iota(jnp.int32, moment_t.shape, 1)
    rate = jnp.where(
        lane < 4, 2.0 * jnp.pi, jnp.where(lane < 6, 4.0 * jnp.pi, 6.0 * jnp.pi))
    phase = rate * moment_t / 365.25
    wave = jnp.where(jnp.bitwise_and(lane, 1) == 0, jnp.cos(phase), jnp.sin(phase))
    linear = (moment_t - 512.0) / 512.0
    return jnp.where(lane == 0, 1.0, jnp.where(lane == 1, linear, wave))


def kernel(dims, stack, quality, days, fin, tot_ref,
           des_in, qbuf, code, raw, dall, bdes, wbuf, lbuf, wsum_ref, res, rel,
           ssum, part, part_date, part_mid, part_pix,
           q_sem, des_send, des_recv, raw_send, raw_recv,
           hop_send, rel_recv, fin_send, fin_recv,
           pd_send, pd_recv, pp_send, pp_recv):
    dates, pixes, times, bands, block = dims
    per = pixes // dates
    units = per // PAIR
    tall = PAIR * block
    s = lax.axis_index("date")
    q = lax.axis_index("pix")
    total = dates * times
    place = lax.rem(q, per)
    home = q // per

    def peer_of(k):
        if dates & (dates - 1):
            return lax.rem(s + k, dates)
        return jnp.bitwise_xor(s, k)

    def group(sd):
        flip = lax.rem(q, 2)
        if dates & (dates - 1):
            return lax.rem(home + flip * (dates // 2) + 2 * dates - sd, dates)
        return jnp.bitwise_xor(jnp.bitwise_xor(home, sd), flip * (dates - 1))

    def far_of(r):
        flip = lax.rem(r, 2)
        if dates & (dates - 1):
            return lax.rem(home + s + dates - flip * (dates // 2), dates)
        return jnp.bitwise_xor(jnp.bitwise_xor(home, s), flip * (dates - 1))

    mine = group(s)

    barrier = pltpu.get_barrier_semaphore()
    for k in range(1, dates):
        pl.semaphore_signal(barrier, inc=1, device_id=(peer_of(k), q),
                            device_id_type=MESH)
    for k in range(1, pixes):
        pl.semaphore_signal(barrier, inc=1, device_id=(s, lax.rem(q + k, pixes)),
                            device_id_type=MESH)

    q_copy = pltpu.make_async_copy(quality, qbuf, q_sem)
    q_copy.start()

    def rows_of(g, u):
        first = (g * units + u) * tall
        return pl.ds(pl.multiple_of(first, tall), tall)

    def mine_at(sd):
        return pl.ds(pl.multiple_of(sd * times, times), times)

    for u in range(units):
        for b in range(bands):
            pltpu.make_async_copy(
                stack.at[:, b, rows_of(mine, u), :], raw.at[u, b, mine_at(s)],
                raw_recv.at[u, b, s]).start()

    des_in[...] = design_lanes([days[r] for r in range(times)])
    q_copy.wait()
    for g in range(dates):
        for u in range(units):
            first = (g * units + u) * tall
            bits = qbuf[:, first:first + tall, :]
            digit = jnp.bitwise_and(jnp.right_shift(bits, 6), 12)
            value = jnp.bitwise_and(jnp.right_shift(jnp.full_like(bits, LEVELS), digit), 15)
            value = jnp.where(jnp.bitwise_and(bits, 8) == 0, value, 0)
            code[g, u] = value.astype(jnp.float32).astype(jnp.bfloat16)

    pl.semaphore_wait(barrier, dates - 1 + pixes - 1)

    def des_copy(k):
        return pltpu.make_async_remote_copy(
            des_in, dall.at[s], des_send.at[k], des_recv.at[s],
            device_id=(peer_of(k), q), device_id_type=MESH)

    def raw_copy(u, b, k):
        peer = peer_of(k)
        return pltpu.make_async_remote_copy(
            stack.at[:, b, rows_of(group(peer), u), :], raw.at[u, b, mine_at(s)],
            raw_send.at[u, b, k], raw_recv.at[u, b, s],
            device_id=(peer, q), device_id_type=MESH)

    def code_copy(u, k):
        peer = peer_of(k)
        return pltpu.make_async_remote_copy(
            code.at[group(peer), u], raw.at[u, bands, mine_at(s)],
            raw_send.at[u, bands, k], raw_recv.at[u, bands, s],
            device_id=(peer, q), device_id_type=MESH)

    order = range(dates - 1, 0, -1)
    for k in order:
        des_copy(k).start()
    for u in range(units):
        for k in order:
            code_copy(u, k).start()
        for b in range(bands):
            for k in order:
                raw_copy(u, b, k).start()
    for u in range(units):
        pltpu.make_async_copy(
            code.at[mine, u], raw.at[u, bands, mine_at(s)],
            raw_recv.at[u, bands, s]).start()

    def raw_wait(u, b, sd):
        there = raw.at[u, b, mine_at(sd)]
        pltpu.make_async_copy(there, there, raw_recv.at[u, b, sd]).wait()

    dall[s] = des_in[...]

    zero = jnp.zeros((PAIR, block, 128), jnp.float32)
    zero_one = jnp.zeros((block, 128), jnp.float32)
    for b in range(bands + 1):
        ssum[b] = zero_one

    def spread(k):
        sd = peer_of(k)
        if k:
            pltpu.make_async_copy(dall.at[sd], dall.at[sd], des_recv.at[sd]).wait()

        @pl.loop(0, times, unroll=4)
        def _(r):
            row = dall[sd, pl.ds(r, 1), :]
            for i in range(HARM):
                bdes[sd * times + r, i] = jnp.broadcast_to(row[:, i:i + 1], (block, 128))

    for k in range(dates):
        spread(k)

    def pair_of(value):
        return value.astype(jnp.float32).reshape(PAIR, block, 128)

    def by_source(wait, body, carry, unroll):
        def source(k, carry):
            sd = peer_of(k)
            wait(sd)
            return lax.fori_loop(
                0, times, lambda r, c: body(sd * times + r, c), carry, unroll=unroll)

        return lax.fori_loop(0, dates, source, carry)

    def gram_step(u):
        def body(jj):
            def step(t, carry):
                if jj == 0:
                    both = pair_of(raw[u, bands, t]) * (1.0 / 12.0)
                    wbuf[t] = both
                    w = both[0]
                else:
                    w = wbuf[t, jj]
                d = [bdes[t, i] for i in range(HARM)]
                wd = [w] + [w * d[i] for i in range(1, HARM)]
                return tuple(
                    carry[n] + (wd[first] if second == 0 else wd[first] * d[second])
                    for n, (first, second) in enumerate(PAIR_LIST))
            return step

        start = (zero_one,) * len(PAIR_LIST)
        gram = by_source(lambda sd: raw_wait(u, bands, sd), body(0), start, 2)
        for n in range(len(PAIR_LIST)):
            lbuf[n, 0] = gram[n]
        for jj in range(1, PAIR):
            gram = lax.fori_loop(0, total, body(jj), start, unroll=2)
            for n in range(len(PAIR_LIST)):
                lbuf[n, jj] = gram[n]
        gram = [lbuf[n] for n in range(len(PAIR_LIST))]
        wsum_ref[...] = 1.0 / (gram[0] + 1.0)
        ssum[bands] = ssum[bands] + jnp.sum(gram[0], 0)
        lower = {}
        for first in range(HARM):
            for second in range(first + 1):
                value = gram[PAIR_AT[first, second]]
                if first == second:
                    value = value + RIDGE_TERM
                for inner in range(second):
                    value = value - lower[first, inner] * lower[second, inner]
                if first == second:
                    lower[first, first] = lax.rsqrt(value)
                else:
                    lower[first, second] = value * lower[second, second]
                lbuf[PAIR_AT[first, second]] = lower[first, second]

    def hop(u, b, start):
        for jj in range(PAIR):
            p = mine * per + PAIR * u + jj

            def act(dst, sem):
                @pl.when(p != q)
                def _():
                    c = pltpu.make_async_remote_copy(
                        res.at[u, b, jj], dst, hop_send.at[u, b, jj], sem,
                        device_id=(s, p), device_id_type=MESH)
                    c.start() if start else c.wait_send()

                if start:
                    @pl.when(p == q)
                    def _():
                        pltpu.make_async_copy(res.at[u, b, jj], dst, sem).start()

            @pl.when(home == s)
            def _():
                act(fin.at[place, b], fin_recv.at[place, b])

            @pl.when(home != s)
            def _():
                act(rel.at[place, b], rel_recv.at[place, b])

    def band_step(u, b):
        def body(t, carry):
            wy = wbuf[t] * pair_of(raw[u, b, t])
            return tuple(
                carry[i] + (wy if i == 0 else bdes[t, i] * wy) for i in range(HARM))

        moment = by_source(lambda sd: raw_wait(u, b, sd), body, (zero,) * HARM, 8)
        low = lambda first, second: lbuf[PAIR_AT[first, second]]
        forward = []
        for first in range(HARM):
            value = moment[first]
            for inner in range(first):
                value = value - low(first, inner) * forward[inner]
            forward.append(value * low(first, first))
        back = [None] * HARM
        for first in range(HARM - 1, -1, -1):
            value = forward[first]
            for inner in range(HARM - 1, first, -1):
                value = value - low(inner, first) * back[inner]
            back[first] = value * low(first, first)

        def residual(t, ssr):
            terms = [back[0]] + [bdes[t, i] * back[i] for i in range(1, HARM)]
            while len(terms) > 1:
                terms = [terms[i] + terms[i + 1] for i in range(0, len(terms), 2)]
            diff = pair_of(raw[u, b, t]) - terms[0]
            return ssr + wbuf[t] * diff * diff

        ssr = lax.fori_loop(0, total, residual, zero, unroll=8)
        ratio = jnp.sqrt(ssr * wsum_ref[...])
        peak = ratio
        for i in range(HARM):
            peak = jnp.maximum(peak, jnp.abs(back[i]))
        level = jnp.ceil(jnp.log2(jnp.maximum(peak, 1e-36)) + 0.01)
        inverse = jnp.exp2(-level)
        scale = inverse * LIMIT
        for i in range(HARM):
            put(res, u, b, i, jnp.floor(jnp.clip(back[i] * scale, -LIMIT, LIMIT) + 0.5))
        root = jnp.sqrt(jnp.sqrt(jnp.minimum(ratio * inverse, 1.0)))
        put(res, u, b, HARM, jnp.floor(root * LIMIT + 0.5))
        put(res, u, b, HARM + 1, level)
        ssum[b] = ssum[b] + jnp.sum(ssr, 0)
        hop(u, b, True)

    def pass_on(r, b, start):
        far = far_of(r)

        @pl.when(far != s)
        def _():
            c = pltpu.make_async_remote_copy(
                rel.at[r, b], fin.at[r, b], fin_send.at[r, b], fin_recv.at[r, b],
                device_id=(far, q), device_id_type=MESH)
            if start:
                pltpu.make_async_copy(rel.at[r, b], rel.at[r, b], rel_recv.at[r, b]).wait()
                c.start()
            else:
                c.wait_send()

    def relay(n):
        b = lax.rem(n, bands)

        @pl.when(n // bands == place // PAIR)
        def _():
            for r in range(per):
                pass_on(r, b, True)

    @pl.loop(0, units * bands)
    def _(n):
        u = n // bands
        b = lax.rem(n, bands)

        @pl.when(b == 0)
        def _():
            gram_step(u)

        band_step(u, b)

        @pl.when(n >= LAG)
        def _():
            relay(n - LAG)

    part[...] = jnp.concatenate(
        [jnp.sum(ssum[b], 0, keepdims=True) for b in range(bands + 1)], 0)

    def date_part(k):
        return pltpu.make_async_remote_copy(
            part, part_date.at[s], pd_send.at[k], pd_recv.at[s],
            device_id=(peer_of(k), q), device_id_type=MESH)

    def pix_part(k):
        return pltpu.make_async_remote_copy(
            part_mid, part_pix.at[q], pp_send.at[k], pp_recv.at[q],
            device_id=(s, lax.rem(q + k, pixes)), device_id_type=MESH)

    for k in range(1, dates):
        date_part(k).start()
    part_date[s] = part[...]
    for n in range(LAG):
        relay(units * bands - LAG + n)
    for k in range(1, dates):
        sd = peer_of(k)
        pltpu.make_async_copy(part_date.at[sd], part_date.at[sd], pd_recv.at[sd]).wait()
    mid = part_date[0]
    for sd in range(1, dates):
        mid = mid + part_date[sd]
    part_mid[...] = mid
    for k in range(1, pixes):
        pix_part(k).start()
    part_pix[q] = mid

    @pl.loop(0, bands)
    def _(b):
        for r in range(per):
            pltpu.make_async_copy(fin.at[r, b], fin.at[r, b], fin_recv.at[r, b]).wait()

    for k in range(1, pixes):
        qq = lax.rem(q + k, pixes)
        pltpu.make_async_copy(part_pix.at[qq], part_pix.at[qq], pp_recv.at[qq]).wait()
    tot = part_pix[0]
    for qq in range(1, pixes):
        tot = tot + part_pix[qq]
    tot_ref[...] = tot

    for k in range(1, dates):
        des_copy(k).wait_send()
        date_part(k).wait_send()
    for k in range(1, pixes):
        pix_part(k).wait_send()

    @pl.loop(0, units)
    def _(u):
        for k in range(1, dates):
            code_copy(u, k).wait_send()

        @pl.loop(0, bands)
        def _(b):
            for k in range(1, dates):
                raw_copy(u, b, k).wait_send()
            hop(u, b, False)

    @pl.loop(0, bands)
    def _(b):
        for r in range(per):
            pass_on(r, b, False)


def put(res, u, b, i, value):
    whole = value.astype(jnp.int32)
    for jj in range(PAIR):
        res[u, b, jj, i] = whole[jj].astype(jnp.int16)


def finish(fin, tot_ref, coef, score):
    per, bands = fin.shape[:2]
    tot = jnp.sum(tot_ref[...], 1, keepdims=True)
    for b in range(bands):
        sigma = jnp.sqrt(tot[b:b + 1] / tot[bands:bands + 1])
        scale = jnp.broadcast_to(1.0 / sigma, fin.shape[3:])
        for r in range(per):
            cols = slice(r * 128, (r + 1) * 128)
            number = lambda i: fin[r, b, i].astype(jnp.int32).astype(jnp.float32)
            unit = jnp.exp2(number(HARM + 1))
            step = unit * (1.0 / LIMIT)
            for i in range(HARM):
                coef[b, i, :, cols] = number(i) * step
            root = number(HARM) * (1.0 / LIMIT)
            root = root * root
            score[b, :, cols] = root * root * (unit * scale)


def local(mesh, stack, quality, days):
    dates, pixes = mesh.shape["date"], mesh.shape["pix"]
    times, bands, rows, width = stack.shape
    block = rows // pixes
    per = pixes // dates
    units = per // PAIR
    total = dates * times
    dims = (dates, pixes, times, bands, block)
    tile = (block, width)
    both = (PAIR,) + tile
    tall = (PAIR * block, width)
    vmem, dma = pltpu.VMEM, pltpu.SemaphoreType.DMA
    f32, bf16 = jnp.float32, jnp.bfloat16
    fin, tot = pl.pallas_call(
        functools.partial(kernel, dims),
        out_shape=(
            jax.ShapeDtypeStruct((per, bands, HARM + 2) + tile, jnp.int16),
            jax.ShapeDtypeStruct((bands + 1, width), f32),
        ),
        in_specs=[
            pl.BlockSpec(memory_space=pl.ANY),
            pl.BlockSpec(memory_space=pl.ANY),
            pl.BlockSpec(memory_space=pltpu.SMEM),
        ],
        out_specs=(
            pl.BlockSpec(memory_space=pl.ANY),
            pl.BlockSpec(memory_space=pltpu.VMEM),
        ),
        scratch_shapes=[
            vmem((times, 128), f32),
            vmem((times, rows, width), jnp.int32),
            vmem((dates, units, times) + tall, bf16),
            vmem((units, bands + 1, total) + tall, bf16),
            vmem((dates, times, 128), f32),
            vmem((total, HARM) + tile, f32),
            vmem((total,) + both, f32),
            vmem((len(PAIR_LIST),) + both, f32),
            vmem(both, f32),
            vmem((units, bands, PAIR, HARM + 2) + tile, jnp.int16),
            vmem((per, bands, HARM + 2) + tile, jnp.int16),
            vmem((bands + 1,) + tile, f32),
            vmem((bands + 1, width), f32),
            vmem((dates, bands + 1, width), f32),
            vmem((bands + 1, width), f32),
            vmem((pixes, bands + 1, width), f32),
            dma,
            dma((dates,)),
            dma((dates,)),
            dma((units, bands + 1, dates)),
            dma((units, bands + 1, dates)),
            dma((units, bands, PAIR)),
            dma((per, bands)),
            dma((per, bands)),
            dma((per, bands)),
            dma((dates,)),
            dma((dates,)),
            dma((pixes,)),
            dma((pixes,)),
        ],
        compiler_params=pltpu.CompilerParams(
            collective_id=0, has_side_effects=True, vmem_limit_bytes=60000000
        ),
    )(stack, quality, days)
    whole = pl.BlockSpec(memory_space=pltpu.VMEM)
    return pl.pallas_call(
        finish,
        out_shape=(
            jax.ShapeDtypeStruct((bands, HARM, block, width * per), f32),
            jax.ShapeDtypeStruct((bands, block, width * per), f32),
        ),
        in_specs=[whole, whole],
        out_specs=(whole, whole),
    )(fin, tot)


def solution(mesh):
    return jax.shard_map(
        functools.partial(local, mesh),
        mesh=mesh,
        in_specs=(P("date", None, None, "pix"), P("date", None, "pix"), P("date")),
        out_specs=(P(None, None, "pix", "date"), P(None, "pix", "date")),
        check_vma=False,
    )
```

```python
import functools

import jax
import jax.numpy as jnp
from jax import lax
from jax.experimental import pallas as pl
from jax.experimental.pallas import tpu as pltpu
from jax.sharding import PartitionSpec as P

RIDGE_TERM = 1.0
HARM = 8
PAIR = 2
LAG = 4
DIRECT = 1
LIMIT = 32767.0
LEVELS = 0x346C

MESH = pl.DeviceIdType.MESH
PAIR_LIST = [(first, second) for first in range(HARM) for second in range(first + 1)]
PAIR_AT = {pair: number for number, pair in enumerate(PAIR_LIST)}


def design_lanes(days):
    rows = [jnp.full((1, 128), day, jnp.int32) for day in days]
    moment_t = jnp.concatenate(rows, 0).astype(jnp.float32)
    lane = lax.broadcasted_iota(jnp.int32, moment_t.shape, 1)
    rate = jnp.where(
        lane < 4, 2.0 * jnp.pi, jnp.where(lane < 6, 4.0 * jnp.pi, 6.0 * jnp.pi))
    phase = rate * moment_t / 365.25
    wave = jnp.where(jnp.bitwise_and(lane, 1) == 0, jnp.cos(phase), jnp.sin(phase))
    linear = (moment_t - 512.0) / 512.0
    return jnp.where(lane == 0, 1.0, jnp.where(lane == 1, linear, wave))


def kernel(dims, stack, quality, days, fin, tot_ref,
           des_in, qbuf, code, raw, dall, bdes, wbuf, lbuf, wsum_ref, res, rel,
           ssum, part, part_all,
           q_sem, des_send, des_recv, raw_send, raw_recv,
           hop_send, rel_recv, fin_send, fin_recv,
           part_send, part_recv):
    dates, pixes, times, bands, block = dims
    per = pixes // dates
    units = per // PAIR
    tall = PAIR * block
    s = lax.axis_index("date")
    q = lax.axis_index("pix")
    total = dates * times
    place = lax.rem(q, per)
    home = q // per

    def peer_of(k):
        if dates & (dates - 1):
            return lax.rem(s + k, dates)
        return jnp.bitwise_xor(s, k)

    def group(sd):
        flip = lax.rem(q, 2)
        if dates & (dates - 1):
            return lax.rem(home + flip * (dates // 2) + 2 * dates - sd, dates)
        return jnp.bitwise_xor(jnp.bitwise_xor(home, sd), flip * (dates - 1))

    def far_of(r):
        flip = lax.rem(r, 2)
        if dates & (dates - 1):
            return lax.rem(home + s + dates - flip * (dates // 2), dates)
        return jnp.bitwise_xor(jnp.bitwise_xor(home, s), flip * (dates - 1))

    mine = group(s)

    barrier = pltpu.get_barrier_semaphore()
    others = [(k, kk) for k in range(dates) for kk in range(pixes) if k or kk]
    for k, kk in others:
        pl.semaphore_signal(barrier, inc=1, device_id=(peer_of(k), lax.rem(q + kk, pixes)),
                            device_id_type=MESH)

    q_copy = pltpu.make_async_copy(quality, qbuf, q_sem)
    q_copy.start()

    def rows_of(g, u):
        first = (g * units + u) * tall
        return pl.ds(pl.multiple_of(first, tall), tall)

    def mine_at(sd):
        return pl.ds(pl.multiple_of(sd * times, times), times)

    for u in range(units):
        for b in range(bands):
            pltpu.make_async_copy(
                stack.at[:, b, rows_of(mine, u), :], raw.at[u, b, mine_at(s)],
                raw_recv.at[u, b, s]).start()

    des_in[...] = design_lanes([days[r] for r in range(times)])
    q_copy.wait()
    for g in range(dates):
        for u in range(units):
            first = (g * units + u) * tall
            bits = qbuf[:, first:first + tall, :]
            digit = jnp.bitwise_and(jnp.right_shift(bits, 6), 12)
            value = jnp.bitwise_and(jnp.right_shift(jnp.full_like(bits, LEVELS), digit), 15)
            value = jnp.where(jnp.bitwise_and(bits, 8) == 0, value, 0)
            code[g, u] = value.astype(jnp.float32).astype(jnp.bfloat16)

    pl.semaphore_wait(barrier, len(others))

    def des_copy(k):
        return pltpu.make_async_remote_copy(
            des_in, dall.at[s], des_send.at[k], des_recv.at[s],
            device_id=(peer_of(k), q), device_id_type=MESH)

    def raw_copy(u, b, k):
        peer = peer_of(k)
        return pltpu.make_async_remote_copy(
            stack.at[:, b, rows_of(group(peer), u), :], raw.at[u, b, mine_at(s)],
            raw_send.at[u, b, k], raw_recv.at[u, b, s],
            device_id=(peer, q), device_id_type=MESH)

    def code_copy(u, k):
        peer = peer_of(k)
        return pltpu.make_async_remote_copy(
            code.at[group(peer), u], raw.at[u, bands, mine_at(s)],
            raw_send.at[u, bands, k], raw_recv.at[u, bands, s],
            device_id=(peer, q), device_id_type=MESH)

    order = range(dates - 1, 0, -1)
    for k in order:
        des_copy(k).start()
    for u in range(units):
        for k in order:
            code_copy(u, k).start()
        for b in range(bands):
            for k in order:
                raw_copy(u, b, k).start()
    for u in range(units):
        pltpu.make_async_copy(
            code.at[mine, u], raw.at[u, bands, mine_at(s)],
            raw_recv.at[u, bands, s]).start()

    def raw_wait(u, b, sd):
        there = raw.at[u, b, mine_at(sd)]
        pltpu.make_async_copy(there, there, raw_recv.at[u, b, sd]).wait()

    dall[s] = des_in[...]

    zero = jnp.zeros((PAIR, block, 128), jnp.float32)
    zero_one = jnp.zeros((block, 128), jnp.float32)
    for b in range(bands + 1):
        ssum[b] = zero_one

    def spread(k):
        sd = peer_of(k)
        if k:
            pltpu.make_async_copy(dall.at[sd], dall.at[sd], des_recv.at[sd]).wait()

        @pl.loop(0, times, unroll=4)
        def _(r):
            row = dall[sd, pl.ds(r, 1), :]
            for i in range(HARM):
                bdes[sd * times + r, i] = jnp.broadcast_to(row[:, i:i + 1], (block, 128))

    for k in range(dates):
        spread(k)

    def pair_of(value):
        return value.astype(jnp.float32).reshape(PAIR, block, 128)

    def by_source(wait, body, carry, unroll):
        def source(k, carry):
            sd = peer_of(k)
            wait(sd)
            return lax.fori_loop(
                0, times, lambda r, c: body(sd * times + r, c), carry, unroll=unroll)

        return lax.fori_loop(0, dates, source, carry)

    def gram_step(u):
        def body(jj):
            def step(t, carry):
                if jj == 0:
                    both = pair_of(raw[u, bands, t]) * (1.0 / 12.0)
                    wbuf[t] = both
                    w = both[0]
                else:
                    w = wbuf[t, jj]
                d = [bdes[t, i] for i in range(HARM)]
                wd = [w] + [w * d[i] for i in range(1, HARM)]
                return tuple(
                    carry[n] + (wd[first] if second == 0 else wd[first] * d[second])
                    for n, (first, second) in enumerate(PAIR_LIST))
            return step

        start = (zero_one,) * len(PAIR_LIST)
        gram = by_source(lambda sd: raw_wait(u, bands, sd), body(0), start, 2)
        for n in range(len(PAIR_LIST)):
            lbuf[n, 0] = gram[n]
        for jj in range(1, PAIR):
            gram = lax.fori_loop(0, total, body(jj), start, unroll=2)
            for n in range(len(PAIR_LIST)):
                lbuf[n, jj] = gram[n]
        gram = [lbuf[n] for n in range(len(PAIR_LIST))]
        wsum_ref[...] = 1.0 / (gram[0] + 1.0)
        ssum[bands] = ssum[bands] + jnp.sum(gram[0], 0)
        lower = {}
        for first in range(HARM):
            for second in range(first + 1):
                value = gram[PAIR_AT[first, second]]
                if first == second:
                    value = value + RIDGE_TERM
                for inner in range(second):
                    value = value - lower[first, inner] * lower[second, inner]
                if first == second:
                    lower[first, first] = lax.rsqrt(value)
                else:
                    lower[first, second] = value * lower[second, second]
                lbuf[PAIR_AT[first, second]] = lower[first, second]

    def hop(u, b, start):
        for jj in range(PAIR):
            p = mine * per + PAIR * u + jj

            def act(dst, sem):
                @pl.when(p != q)
                def _():
                    c = pltpu.make_async_remote_copy(
                        res.at[u, b, jj], dst, hop_send.at[u, b, jj], sem,
                        device_id=(s, p), device_id_type=MESH)
                    c.start() if start else c.wait_send()

                if start:
                    @pl.when(p == q)
                    def _():
                        pltpu.make_async_copy(res.at[u, b, jj], dst, sem).start()

            @pl.when(home == s)
            def _():
                act(fin.at[place, b], fin_recv.at[place, b])

            late = u * bands + b >= units * bands - DIRECT

            @pl.when(jnp.logical_and(home != s, jnp.logical_not(late)))
            def _():
                act(rel.at[place, b], rel_recv.at[place, b])

            @pl.when(jnp.logical_and(home != s, late))
            def _():
                c = pltpu.make_async_remote_copy(
                    res.at[u, b, jj], fin.at[place, b], hop_send.at[u, b, jj],
                    fin_recv.at[place, b], device_id=(home, p), device_id_type=MESH)
                c.start() if start else c.wait_send()

    def band_step(u, b):
        def body(t, carry):
            wy = wbuf[t] * pair_of(raw[u, b, t])
            return tuple(
                carry[i] + (wy if i == 0 else bdes[t, i] * wy) for i in range(HARM))

        moment = by_source(lambda sd: raw_wait(u, b, sd), body, (zero,) * HARM, 8)
        low = lambda first, second: lbuf[PAIR_AT[first, second]]
        forward = []
        for first in range(HARM):
            value = moment[first]
            for inner in range(first):
                value = value - low(first, inner) * forward[inner]
            forward.append(value * low(first, first))
        back = [None] * HARM
        for first in range(HARM - 1, -1, -1):
            value = forward[first]
            for inner in range(HARM - 1, first, -1):
                value = value - low(inner, first) * back[inner]
            back[first] = value * low(first, first)

        def residual(t, ssr):
            terms = [back[0]] + [bdes[t, i] * back[i] for i in range(1, HARM)]
            while len(terms) > 1:
                terms = [terms[i] + terms[i + 1] for i in range(0, len(terms), 2)]
            diff = pair_of(raw[u, b, t]) - terms[0]
            return ssr + wbuf[t] * diff * diff

        ssr = lax.fori_loop(0, total, residual, zero, unroll=8)
        ratio = jnp.sqrt(ssr * wsum_ref[...])
        peak = ratio
        for i in range(HARM):
            peak = jnp.maximum(peak, jnp.abs(back[i]))
        level = jnp.ceil(jnp.log2(jnp.maximum(peak, 1e-36)) + 0.01)
        inverse = jnp.exp2(-level)
        scale = inverse * LIMIT
        for i in range(HARM):
            put(res, u, b, i, jnp.floor(jnp.clip(back[i] * scale, -LIMIT, LIMIT) + 0.5))
        root = jnp.sqrt(jnp.sqrt(jnp.minimum(ratio * inverse, 1.0)))
        put(res, u, b, HARM, jnp.floor(root * LIMIT + 0.5))
        put(res, u, b, HARM + 1, level)
        ssum[b] = ssum[b] + jnp.sum(ssr, 0)
        hop(u, b, True)

    def pass_on(r, b, start):
        far = far_of(r)

        @pl.when(far != s)
        def _():
            c = pltpu.make_async_remote_copy(
                rel.at[r, b], fin.at[r, b], fin_send.at[r, b], fin_recv.at[r, b],
                device_id=(far, q), device_id_type=MESH)
            if start:
                pltpu.make_async_copy(rel.at[r, b], rel.at[r, b], rel_recv.at[r, b]).wait()
                c.start()
            else:
                c.wait_send()

    def relay(n):
        b = lax.rem(n, bands)

        @pl.when(n // bands == place // PAIR)
        def _():
            for r in range(per):
                pass_on(r, b, True)

    @pl.loop(0, units * bands)
    def _(n):
        u = n // bands
        b = lax.rem(n, bands)

        @pl.when(b == 0)
        def _():
            gram_step(u)

        band_step(u, b)

        @pl.when(n >= LAG)
        def _():
            relay(n - LAG)

    sums = jnp.concatenate(
        [jnp.sum(ssum[b], 0, keepdims=True) for b in range(bands + 1)], 0)
    sums = jnp.broadcast_to(jnp.sum(sums, 1, keepdims=True), sums.shape)
    lane = lax.broadcasted_iota(jnp.int32, sums.shape, 1)
    row = lax.broadcasted_iota(jnp.int32, sums.shape, 0)
    part[...] = jnp.sum(jnp.where(lane == row, sums, 0.0), 0, keepdims=True)
    here = s * pixes + q

    def part_copy(k, kk):
        return pltpu.make_async_remote_copy(
            part, part_all.at[here], part_send.at[k, kk], part_recv.at[here],
            device_id=(peer_of(k), lax.rem(q + kk, pixes)), device_id_type=MESH)

    for k, kk in others:
        part_copy(k, kk).start()
    part_all[here] = part[...]
    for n in range(LAG, DIRECT, -1):
        relay(units * bands - n)

    @pl.loop(0, bands)
    def _(b):
        for r in range(per):
            pltpu.make_async_copy(fin.at[r, b], fin.at[r, b], fin_recv.at[r, b]).wait()

    for k, kk in others:
        there = peer_of(k) * pixes + lax.rem(q + kk, pixes)
        pltpu.make_async_copy(part_all.at[there], part_all.at[there], part_recv.at[there]).wait()
    terms = [part_all[n] for n in range(dates * pixes)]
    while len(terms) > 1:
        terms = [sum(terms[i:i + 2]) for i in range(0, len(terms), 2)]
    tot_ref[...] = terms[0]

    for k in range(1, dates):
        des_copy(k).wait_send()
    for k, kk in others:
        part_copy(k, kk).wait_send()

    @pl.loop(0, units)
    def _(u):
        for k in range(1, dates):
            code_copy(u, k).wait_send()

        @pl.loop(0, bands)
        def _(b):
            for k in range(1, dates):
                raw_copy(u, b, k).wait_send()
            hop(u, b, False)

    @pl.loop(0, bands)
    def _(b):
        @pl.when((place // PAIR) * bands + b < units * bands - DIRECT)
        def _():
            for r in range(per):
                pass_on(r, b, False)


def put(res, u, b, i, value):
    whole = value.astype(jnp.int32)
    for jj in range(PAIR):
        res[u, b, jj, i] = whole[jj].astype(jnp.int16)


def finish(fin, tot_ref, coef, score, coef_buf, score_buf, coef_sem, score_sem):
    per, bands = fin.shape[:2]
    copies = []
    tot = tot_ref[...]
    for b in range(bands):
        sigma = jnp.sqrt(tot[:, b:b + 1] / tot[:, bands:bands + 1])
        scale = jnp.broadcast_to(1.0 / sigma, fin.shape[3:])
        for r in range(per):
            cols = slice(r * 128, (r + 1) * 128)
            number = lambda i: fin[r, b, i].astype(jnp.int32).astype(jnp.float32)
            unit = jnp.exp2(number(HARM + 1))
            step = unit * (1.0 / LIMIT)
            for i in range(HARM):
                coef_buf[b, i, :, cols] = number(i) * step
            root = number(HARM) * (1.0 / LIMIT)
            root = root * root
            score_buf[b, :, cols] = root * root * (unit * scale)
        copies.append(pltpu.make_async_copy(coef_buf.at[b], coef.at[b], coef_sem.at[b]))
        copies[-1].start()
    copies.append(pltpu.make_async_copy(score_buf, score, score_sem))
    copies[-1].start()
    for c in copies:
        c.wait()


def local(mesh, stack, quality, days):
    dates, pixes = mesh.shape["date"], mesh.shape["pix"]
    times, bands, rows, width = stack.shape
    block = rows // pixes
    per = pixes // dates
    units = per // PAIR
    total = dates * times
    dims = (dates, pixes, times, bands, block)
    tile = (block, width)
    both = (PAIR,) + tile
    tall = (PAIR * block, width)
    vmem, dma = pltpu.VMEM, pltpu.SemaphoreType.DMA
    f32, bf16 = jnp.float32, jnp.bfloat16
    fin, tot = pl.pallas_call(
        functools.partial(kernel, dims),
        out_shape=(
            vmem((per, bands, HARM + 2) + tile, jnp.int16),
            vmem((1, width), f32),
        ),
        in_specs=[
            pl.BlockSpec(memory_space=pl.ANY),
            pl.BlockSpec(memory_space=pl.ANY),
            pl.BlockSpec(memory_space=pltpu.SMEM),
        ],
        out_specs=(
            pl.BlockSpec(memory_space=pltpu.VMEM),
            pl.BlockSpec(memory_space=pltpu.VMEM),
        ),
        scratch_shapes=[
            vmem((times, 128), f32),
            vmem((times, rows, width), jnp.int32),
            vmem((dates, units, times) + tall, bf16),
            vmem((units, bands + 1, total) + tall, bf16),
            vmem((dates, times, 128), f32),
            vmem((total, HARM) + tile, f32),
            vmem((total,) + both, f32),
            vmem((len(PAIR_LIST),) + both, f32),
            vmem(both, f32),
            vmem((units, bands, PAIR, HARM + 2) + tile, jnp.int16),
            vmem((per, bands, HARM + 2) + tile, jnp.int16),
            vmem((bands + 1,) + tile, f32),
            vmem((1, width), f32),
            vmem((dates * pixes, 1, width), f32),
            dma,
            dma((dates,)),
            dma((dates,)),
            dma((units, bands + 1, dates)),
            dma((units, bands + 1, dates)),
            dma((units, bands, PAIR)),
            dma((per, bands)),
            dma((per, bands)),
            dma((per, bands)),
            dma((dates, pixes)),
            dma((dates * pixes,)),
        ],
        compiler_params=pltpu.CompilerParams(
            collective_id=0, has_side_effects=True, vmem_limit_bytes=60000000
        ),
    )(stack, quality, days)
    whole = pl.BlockSpec(memory_space=pltpu.VMEM)
    there = pl.BlockSpec(memory_space=pl.ANY)
    coef_shape = (bands, HARM, block, width * per)
    score_shape = (bands, block, width * per)
    return pl.pallas_call(
        finish,
        out_shape=(
            jax.ShapeDtypeStruct(coef_shape, f32),
            jax.ShapeDtypeStruct(score_shape, f32),
        ),
        in_specs=[whole, whole],
        out_specs=(there, there),
        scratch_shapes=[vmem(coef_shape, f32), vmem(score_shape, f32), dma((bands,)), dma],
        compiler_params=pltpu.CompilerParams(vmem_limit_bytes=20000000),
    )(fin, tot)


def solution(mesh):
    return jax.shard_map(
        functools.partial(local, mesh),
        mesh=mesh,
        in_specs=(P("date", None, None, "pix"), P("date", None, "pix"), P("date")),
        out_specs=(P(None, None, "pix", "date"), P(None, "pix", "date")),
        check_vma=False,
    )
```

```python
import functools

import jax
import jax.numpy as jnp
from jax import lax
from jax.experimental import pallas as pl
from jax.experimental.pallas import tpu as pltpu
from jax.sharding import PartitionSpec as P

RIDGE_TERM = 1.0
HARM = 8
PAIR = 2
LAG = 4
DIRECT = 1
MERGED = 6
REST_AT = 5
BEHIND = 4
GRAM_AT = 2
LIMIT = 32767.0
LEVELS = 0x346C

MESH = pl.DeviceIdType.MESH
PAIR_LIST = [(first, second) for first in range(HARM) for second in range(first + 1)]
PAIR_AT = {pair: number for number, pair in enumerate(PAIR_LIST)}


def design_lanes(days):
    rows = [jnp.full((1, 128), day, jnp.int32) for day in days]
    moment_t = jnp.concatenate(rows, 0).astype(jnp.float32)
    lane = lax.broadcasted_iota(jnp.int32, moment_t.shape, 1)
    rate = jnp.where(
        lane < 4, 2.0 * jnp.pi, jnp.where(lane < 6, 4.0 * jnp.pi, 6.0 * jnp.pi))
    phase = rate * moment_t / 365.25
    wave = jnp.where(jnp.bitwise_and(lane, 1) == 0, jnp.cos(phase), jnp.sin(phase))
    linear = (moment_t - 512.0) / 512.0
    return jnp.where(lane == 0, 1.0, jnp.where(lane == 1, linear, wave))


def kernel(dims, stack, quality, days, fin, tot_ref,
           des_in, qbuf, code, raw, side, dall, bdes, wbuf, wside, gbuf, lbuf, lside,
           wsum_ref, note_out, note_in, res, rel, ssum, part, part_all,
           q_sem, des_send, des_recv, raw_send, raw_recv, side_send, side_recv,
           next_send, note_send, note_recv, hop_send, rel_recv, fin_send, fin_recv,
           part_send, part_recv):
    dates, pixes, times, bands, block = dims
    per = pixes // dates
    units = per // PAIR
    tall = PAIR * block
    s = lax.axis_index("date")
    q = lax.axis_index("pix")
    total = dates * times
    place = lax.rem(q, per)
    home = q // per
    merged = merged_bands(dates, bands)
    along = 1 + lax.rem(q, 2)
    across = 3 - along

    def peer_of(k):
        if dates & (dates - 1):
            return lax.rem(s + k, dates)
        return jnp.bitwise_xor(s, k)

    def group(sd):
        flip = lax.rem(q, 2)
        if dates & (dates - 1):
            return lax.rem(home + flip * (dates // 2) + 2 * dates - sd, dates)
        return jnp.bitwise_xor(jnp.bitwise_xor(home, sd), flip * (dates - 1))

    def far_of(r):
        flip = lax.rem(r, 2)
        if dates & (dates - 1):
            return lax.rem(home + s + dates - flip * (dates // 2), dates)
        return jnp.bitwise_xor(jnp.bitwise_xor(home, s), flip * (dates - 1))

    mine = group(s)

    barrier = pltpu.get_barrier_semaphore()
    others = [(k, kk) for k in range(dates) for kk in range(pixes) if k or kk]
    for k, kk in others:
        pl.semaphore_signal(barrier, inc=1, device_id=(peer_of(k), lax.rem(q + kk, pixes)),
                            device_id_type=MESH)

    q_copy = pltpu.make_async_copy(quality, qbuf, q_sem)
    q_copy.start()

    def rows_of(g, u):
        first = (g * units + u) * tall
        return pl.ds(pl.multiple_of(first, tall), tall)

    def mine_at(sd):
        return pl.ds(pl.multiple_of(sd * times, times), times)

    for u in range(units):
        for b in range(bands):
            pltpu.make_async_copy(
                stack.at[:, b, rows_of(mine, u), :], raw.at[u, b, mine_at(s)],
                raw_recv.at[u, b, s]).start()
            if b < merged:
                pltpu.make_async_copy(
                    stack.at[:, b, rows_of(group(peer_of(along)), u), :],
                    side.at[u, b, pl.ds(0, times)], side_recv.at[u, b, 0]).start()

    des_in[...] = design_lanes([days[r] for r in range(times)])
    q_copy.wait()
    for g in range(dates):
        for u in range(units):
            first = (g * units + u) * tall
            bits = qbuf[:, first:first + tall, :]
            digit = jnp.bitwise_and(jnp.right_shift(bits, 6), 12)
            value = jnp.bitwise_and(jnp.right_shift(jnp.full_like(bits, LEVELS), digit), 15)
            value = jnp.where(jnp.bitwise_and(bits, 8) == 0, value, 0)
            code[g, u] = value.astype(jnp.float32).astype(jnp.bfloat16)

    pl.semaphore_wait(barrier, len(others))

    def des_copy(k):
        return pltpu.make_async_remote_copy(
            des_in, dall.at[s], des_send.at[k], des_recv.at[s],
            device_id=(peer_of(k), q), device_id_type=MESH)

    def values_of(u, b, k):
        return stack.at[:, b, rows_of(group(peer_of(k)), u), :]

    def codes_of(u, k):
        return code.at[group(peer_of(k)), u]

    def raw_copy(src, u, b, k, slot):
        return pltpu.make_async_remote_copy(
            src, raw.at[u, b, mine_at(s)], raw_send.at[u, b, slot], raw_recv.at[u, b, s],
            device_id=(peer_of(k), q), device_id_type=MESH)

    def side_copy(src, u, b):
        return pltpu.make_async_remote_copy(
            src, side.at[u, b, pl.ds(times, times)], side_send.at[u, b], side_recv.at[u, b, 1],
            device_id=(peer_of(across), q), device_id_type=MESH)

    def next_copy(u):
        first = peer_of(across)
        return pltpu.make_async_remote_copy(
            side.at[u, merged, pl.ds(times, times)], raw.at[u, bands, mine_at(first)],
            next_send.at[u], raw_recv.at[u, bands, first],
            device_id=(peer_of(along), q), device_id_type=MESH)

    def note_copy(u, b):
        return pltpu.make_async_remote_copy(
            note_out.at[u, b], note_in.at[u, b], note_send.at[u, b], note_recv.at[u, b],
            device_id=(peer_of(along), q), device_id_type=MESH)

    order = list(range(dates - 1, 0, -1))

    def code_copies(u):
        if not merged:
            return [raw_copy(codes_of(u, k), u, bands, k, k) for k in order]
        return [side_copy(codes_of(u, dates - 1), u, merged),
                raw_copy(codes_of(u, across), u, bands, across, 1),
                raw_copy(codes_of(u, along), u, bands, along, 2)]

    def merged_copies(u, b):
        return [side_copy(values_of(u, b, dates - 1), u, b),
                raw_copy(values_of(u, b, across), u, b, across, 1)]

    def rest_copies(u, b):
        return [raw_copy(values_of(u, b, k), u, b, k, k) for k in order]

    for k in order:
        des_copy(k).start()
    for u in range(units):
        for c in code_copies(u):
            c.start()
        for b in range(merged):
            for c in merged_copies(u, b):
                c.start()
        if not merged:
            for b in range(bands):
                for c in rest_copies(u, b):
                    c.start()
    for u in range(units):
        pltpu.make_async_copy(
            code.at[mine, u], raw.at[u, bands, mine_at(s)],
            raw_recv.at[u, bands, s]).start()
        if merged:
            pltpu.make_async_copy(
                code.at[group(peer_of(along)), u], side.at[u, merged, pl.ds(0, times)],
                side_recv.at[u, merged, 0]).start()

    def raw_wait(u, b, sd):
        there = raw.at[u, b, mine_at(sd)]
        pltpu.make_async_copy(there, there, raw_recv.at[u, b, sd]).wait()

    dall[s] = des_in[...]

    zero = jnp.zeros((PAIR, block, 128), jnp.float32)
    zero_one = jnp.zeros((block, 128), jnp.float32)
    for b in range(bands + 1):
        ssum[b] = zero_one

    def side_wait(u, b, slot):
        there = side.at[u, b, pl.ds(pl.multiple_of(slot * times, times), times)]
        pltpu.make_async_copy(there, there, side_recv.at[u, b, slot]).wait()

    def spread(k, wait):
        sd = peer_of(k)
        if wait:
            pltpu.make_async_copy(dall.at[sd], dall.at[sd], des_recv.at[sd]).wait()

        rows = dall[sd]
        for i in range(HARM):
            bdes[i, mine_at(sd), :] = jnp.broadcast_to(rows[:, i:i + 1], rows.shape)

    def design(t, i):
        return jnp.broadcast_to(bdes[i, pl.ds(t, 1), :], (block, 128))

    def pair_of(value):
        return value.astype(jnp.float32).reshape(PAIR, block, 128)

    def by_source(count, source_of, wait, body, carry, unroll):
        def source(n, carry):
            sd = source_of(n)
            wait(n, sd)
            return lax.fori_loop(
                0, times, lambda r, c: body(sd * times + r, n * times + r, c), carry,
                unroll=unroll)

        return lax.fori_loop(0, count, source, carry)

    every = (dates, peer_of)
    near = (2, lambda n: peer_of(n * across)) if merged else every
    far = (2, lambda n: peer_of(along + n * (dates - 1 - along)))

    def gram_over(sources, wait, code_at, weight_at, weight_to, out):
        def body(jj):
            def step(t, place_t, carry):
                if jj == 0:
                    both = pair_of(code_at(t, place_t)) * (1.0 / 12.0)
                    weight_to(t, place_t, both)
                    w = both[0]
                else:
                    w = weight_at(t, place_t, jj)
                d = [design(t, i) for i in range(HARM)]
                wd = [w] + [w * d[i] for i in range(1, HARM)]
                return tuple(
                    carry[n] + (wd[first] if second == 0 else wd[first] * d[second])
                    for n, (first, second) in enumerate(PAIR_LIST))
            return step

        start = (zero_one,) * len(PAIR_LIST)
        for jj in range(PAIR):
            gram = by_source(
                *sources, wait if jj == 0 else lambda n, sd: None, body(jj), start, 2)
            for n in range(len(PAIR_LIST)):
                out[n, jj] = gram[n]

    def factor(gram, out):
        lower = {}
        for first in range(HARM):
            for second in range(first + 1):
                value = gram[PAIR_AT[first, second]]
                if first == second:
                    value = value + RIDGE_TERM
                for inner in range(second):
                    value = value - lower[first, inner] * lower[second, inner]
                if first == second:
                    lower[first, first] = lax.rsqrt(value)
                else:
                    lower[first, second] = value * lower[second, second]
                out[PAIR_AT[first, second]] = lower[first, second]

    def solve(moment, lref):
        low = lambda first, second: lref[PAIR_AT[first, second]]
        forward = []
        for first in range(HARM):
            value = moment[first]
            for inner in range(first):
                value = value - low(first, inner) * forward[inner]
            forward.append(value * low(first, first))
        back = [None] * HARM
        for first in range(HARM - 1, -1, -1):
            value = forward[first]
            for inner in range(HARM - 1, first, -1):
                value = value - low(inner, first) * back[inner]
            back[first] = value * low(first, first)
        return back

    def moment_over(sources, wait, value_at, weight_at):
        def body(t, place_t, carry):
            wy = weight_at(t, place_t) * pair_of(value_at(t, place_t))
            return tuple(
                carry[i] + (wy if i == 0 else design(t, i) * wy) for i in range(HARM))

        return by_source(*sources, wait, body, (zero,) * HARM, 8)

    def residual_over(sources, back, value_at, weight_at):
        def body(t, place_t, ssr):
            terms = [back[0]] + [design(t, i) * back[i] for i in range(1, HARM)]
            while len(terms) > 1:
                terms = [terms[i] + terms[i + 1] for i in range(0, len(terms), 2)]
            diff = pair_of(value_at(t, place_t)) - terms[0]
            return ssr + weight_at(t, place_t) * diff * diff

        return by_source(*sources, lambda n, sd: None, body, zero, 8)

    def side_gram(u):
        def wait(n, sd):
            side_wait(u, merged, n)

            @pl.when(n == 1)
            def _():
                next_copy(u).start()

        def keep(t, place_t, both):
            wside[place_t] = both

        gram_over(near, wait, lambda t, place_t: side[u, merged, place_t],
                  lambda t, place_t, jj: wside[place_t, jj], keep, lside)
        factor([lside[n] for n in range(len(PAIR_LIST))], lside)

    def side_step(u, b):
        value_at = lambda t, place_t: side[u, b, place_t]
        weight_at = lambda t, place_t: wside[place_t]
        moment = moment_over(near, lambda n, sd: side_wait(u, b, n), value_at, weight_at)
        back = solve(moment, lside)
        for i in range(HARM):
            note_out[u, b, i] = back[i]
        note_out[u, b, HARM] = residual_over(near, back, value_at, weight_at)
        note_copy(u, b).start()

    def own_gram(u):
        def keep(t, place_t, both):
            wbuf[t] = both

        def over(sources, out):
            gram_over(sources, lambda n, sd: raw_wait(u, bands, sd),
                      lambda t, place_t: raw[u, bands, t],
                      lambda t, place_t, jj: wbuf[t, jj], keep, out)

        over(near, lbuf)
        if merged:
            over(far, gbuf)
            gram = [lbuf[n] + gbuf[n] for n in range(len(PAIR_LIST))]
        else:
            gram = [lbuf[n] for n in range(len(PAIR_LIST))]
        wsum_ref[...] = 1.0 / (gram[0] + 1.0)
        ssum[bands] = ssum[bands] + jnp.sum(gram[0], 0)
        factor(gram, lbuf)

    def far_gram_times(vector):
        rows = []
        for first in range(HARM):
            row = None
            for second in range(HARM):
                pair = (max(first, second), min(first, second))
                term = gbuf[PAIR_AT[pair]] * vector[second]
                row = term if row is None else row + term
            rows.append(row)
        return rows

    def hop(u, b, start):
        for jj in range(PAIR):
            p = mine * per + PAIR * u + jj

            def act(dst, sem):
                @pl.when(p != q)
                def _():
                    c = pltpu.make_async_remote_copy(
                        res.at[u, b, jj], dst, hop_send.at[u, b, jj], sem,
                        device_id=(s, p), device_id_type=MESH)
                    c.start() if start else c.wait_send()

                if start:
                    @pl.when(p == q)
                    def _():
                        pltpu.make_async_copy(res.at[u, b, jj], dst, sem).start()

            @pl.when(home == s)
            def _():
                act(fin.at[place, b], fin_recv.at[place, b])

            late = u * bands + b >= units * bands - DIRECT

            @pl.when(jnp.logical_and(home != s, jnp.logical_not(late)))
            def _():
                act(rel.at[place, b], rel_recv.at[place, b])

            @pl.when(jnp.logical_and(home != s, late))
            def _():
                c = pltpu.make_async_remote_copy(
                    res.at[u, b, jj], fin.at[place, b], hop_send.at[u, b, jj],
                    fin_recv.at[place, b], device_id=(home, p), device_id_type=MESH)
                c.start() if start else c.wait_send()

    def band_step(u, b, with_note):
        value_at = lambda t, place_t: raw[u, b, t]
        weight_at = lambda t, place_t: wbuf[t]
        sources = near if with_note else every
        moment = moment_over(
            sources, lambda n, sd: raw_wait(u, b, sd), value_at, weight_at)
        if with_note:
            pltpu.make_async_copy(note_in.at[u, b], note_in.at[u, b], note_recv.at[u, b]).wait()
            fit = [note_in[u, b, i] for i in range(HARM)]
            rows = far_gram_times(fit)
            moment = [moment[i] + (rows[i] + fit[i]) for i in range(HARM)]
        back = solve(moment, lbuf)
        ssr = residual_over(sources, back, value_at, weight_at)
        if with_note:
            fit = [note_in[u, b, i] for i in range(HARM)]
            shift = [back[i] - fit[i] for i in range(HARM)]
            rows = far_gram_times(shift)
            extra = note_in[u, b, HARM]
            for i in range(HARM):
                extra = extra + shift[i] * (rows[i] - 2.0 * fit[i])
            ssr = jnp.maximum(ssr + extra, 0.0)
        ratio = jnp.sqrt(ssr * wsum_ref[...])
        peak = ratio
        for i in range(HARM):
            peak = jnp.maximum(peak, jnp.abs(back[i]))
        level = jnp.ceil(jnp.log2(jnp.maximum(peak, 1e-36)) + 0.01)
        inverse = jnp.exp2(-level)
        scale = inverse * LIMIT
        for i in range(HARM):
            put(res, u, b, i, jnp.floor(jnp.clip(back[i] * scale, -LIMIT, LIMIT) + 0.5))
        root = jnp.sqrt(jnp.sqrt(jnp.minimum(ratio * inverse, 1.0)))
        put(res, u, b, HARM, jnp.floor(root * LIMIT + 0.5))
        put(res, u, b, HARM + 1, level)
        ssum[b] = ssum[b] + jnp.sum(ssr, 0)
        hop(u, b, True)

    def pass_on(r, b, start):
        far = far_of(r)

        @pl.when(far != s)
        def _():
            c = pltpu.make_async_remote_copy(
                rel.at[r, b], fin.at[r, b], fin_send.at[r, b], fin_recv.at[r, b],
                device_id=(far, q), device_id_type=MESH)
            if start:
                pltpu.make_async_copy(rel.at[r, b], rel.at[r, b], rel_recv.at[r, b]).wait()
                c.start()
            else:
                c.wait_send()

    def relay(n):
        b = lax.rem(n, bands)

        @pl.when(n // bands == place // PAIR)
        def _():
            for r in range(per):
                pass_on(r, b, True)

    def rest_at(u, act):
        for b in range(merged, bands):
            for c in rest_copies(u, b):
                act(c)

    if merged:
        spread(0, False)
        spread(across, True)
    else:
        for k in range(dates):
            spread(k, k > 0)

    behind = BEHIND if merged else 1
    gram_at = GRAM_AT if merged else 0
    steps = bands + behind

    @pl.loop(0, units * steps)
    def _(n):
        u = n // steps
        step = lax.rem(n, steps)
        if merged:
            @pl.when(step == 0)
            def _():
                side_gram(u)

            @pl.when(step < merged)
            def _():
                side_step(u, step)

            @pl.when(n == 0)
            def _():
                spread(along, True)
                spread(dates - 1, True)

            @pl.when(step == REST_AT)
            def _():
                rest_at(u, lambda c: c.start())

        @pl.when(step == gram_at)
        def _():
            own_gram(u)

        b = step - behind
        if merged:
            @pl.when(jnp.logical_and(b >= 0, b < merged))
            def _():
                band_step(u, b, True)

        if merged < bands:
            @pl.when(b >= merged)
            def _():
                band_step(u, b, False)

        done = u * bands + b

        @pl.when(jnp.logical_and(b >= 0, done >= LAG))
        def _():
            relay(done - LAG)

    sums = jnp.concatenate(
        [jnp.sum(ssum[b], 0, keepdims=True) for b in range(bands + 1)], 0)
    sums = jnp.broadcast_to(jnp.sum(sums, 1, keepdims=True), sums.shape)
    lane = lax.broadcasted_iota(jnp.int32, sums.shape, 1)
    row = lax.broadcasted_iota(jnp.int32, sums.shape, 0)
    part[...] = jnp.sum(jnp.where(lane == row, sums, 0.0), 0, keepdims=True)
    here = s * pixes + q

    def part_copy(k, kk):
        return pltpu.make_async_remote_copy(
            part, part_all.at[here], part_send.at[k, kk], part_recv.at[here],
            device_id=(peer_of(k), lax.rem(q + kk, pixes)), device_id_type=MESH)

    for k, kk in others:
        part_copy(k, kk).start()
    part_all[here] = part[...]
    for n in range(LAG, DIRECT, -1):
        relay(units * bands - n)

    @pl.loop(0, bands)
    def _(b):
        for r in range(per):
            pltpu.make_async_copy(fin.at[r, b], fin.at[r, b], fin_recv.at[r, b]).wait()

    for k, kk in others:
        there = peer_of(k) * pixes + lax.rem(q + kk, pixes)
        pltpu.make_async_copy(part_all.at[there], part_all.at[there], part_recv.at[there]).wait()
    terms = [part_all[n] for n in range(dates * pixes)]
    while len(terms) > 1:
        terms = [sum(terms[i:i + 2]) for i in range(0, len(terms), 2)]
    tot_ref[...] = terms[0]

    for k in range(1, dates):
        des_copy(k).wait_send()
    for k, kk in others:
        part_copy(k, kk).wait_send()

    @pl.loop(0, units)
    def _(u):
        for c in code_copies(u):
            c.wait_send()
        if merged:
            next_copy(u).wait_send()

            @pl.loop(0, merged)
            def _(b):
                for c in merged_copies(u, b):
                    c.wait_send()
                note_copy(u, b).wait_send()
            rest_at(u, lambda c: c.wait_send())
        else:
            @pl.loop(0, bands)
            def _(b):
                for c in rest_copies(u, b):
                    c.wait_send()

        @pl.loop(0, bands)
        def _(b):
            hop(u, b, False)

    @pl.loop(0, bands)
    def _(b):
        @pl.when((place // PAIR) * bands + b < units * bands - DIRECT)
        def _():
            for r in range(per):
                pass_on(r, b, False)


def merged_bands(dates, bands):
    return min(MERGED, bands - 1) if dates == 4 else 0


def put(res, u, b, i, value):
    whole = value.astype(jnp.int32)
    for jj in range(PAIR):
        res[u, b, jj, i] = whole[jj].astype(jnp.int16)


def finish(fin, tot_ref, coef, score, coef_buf, score_buf, coef_sem, score_sem):
    per, bands = fin.shape[:2]
    copies = []
    tot = tot_ref[...]
    for b in range(bands):
        sigma = jnp.sqrt(tot[:, b:b + 1] / tot[:, bands:bands + 1])
        scale = jnp.broadcast_to(1.0 / sigma, fin.shape[3:])
        for r in range(per):
            cols = slice(r * 128, (r + 1) * 128)
            number = lambda i: fin[r, b, i].astype(jnp.int32).astype(jnp.float32)
            unit = jnp.exp2(number(HARM + 1))
            step = unit * (1.0 / LIMIT)
            for i in range(HARM):
                coef_buf[b, i, :, cols] = number(i) * step
            root = number(HARM) * (1.0 / LIMIT)
            root = root * root
            score_buf[b, :, cols] = root * root * (unit * scale)
        copies.append(pltpu.make_async_copy(coef_buf.at[b], coef.at[b], coef_sem.at[b]))
        copies[-1].start()
    copies.append(pltpu.make_async_copy(score_buf, score, score_sem))
    copies[-1].start()
    for c in copies:
        c.wait()


def local(mesh, stack, quality, days):
    dates, pixes = mesh.shape["date"], mesh.shape["pix"]
    times, bands, rows, width = stack.shape
    block = rows // pixes
    per = pixes // dates
    units = per // PAIR
    total = dates * times
    dims = (dates, pixes, times, bands, block)
    merged = merged_bands(dates, bands)
    notes = max(merged, 1)
    tile = (block, width)
    both = (PAIR,) + tile
    tall = (PAIR * block, width)
    vmem, dma = pltpu.VMEM, pltpu.SemaphoreType.DMA
    f32, bf16 = jnp.float32, jnp.bfloat16
    fin, tot = pl.pallas_call(
        functools.partial(kernel, dims),
        out_shape=(
            vmem((per, bands, HARM + 2) + tile, jnp.int16),
            vmem((1, width), f32),
        ),
        in_specs=[
            pl.BlockSpec(memory_space=pl.ANY),
            pl.BlockSpec(memory_space=pl.ANY),
            pl.BlockSpec(memory_space=pltpu.SMEM),
        ],
        out_specs=(
            pl.BlockSpec(memory_space=pltpu.VMEM),
            pl.BlockSpec(memory_space=pltpu.VMEM),
        ),
        scratch_shapes=[
            vmem((times, 128), f32),
            vmem((times, rows, width), jnp.int32),
            vmem((dates, units, times) + tall, bf16),
            vmem((units, bands + 1, total) + tall, bf16),
            vmem((units, merged + 1, 2 * times) + tall, bf16),
            vmem((dates, times, 128), f32),
            vmem((HARM, total, width), f32),
            vmem((total,) + both, f32),
            vmem((2 * times,) + both, f32),
            vmem((len(PAIR_LIST),) + both, f32),
            vmem((len(PAIR_LIST),) + both, f32),
            vmem((len(PAIR_LIST),) + both, f32),
            vmem(both, f32),
            vmem((units, notes, HARM + 1) + both, f32),
            vmem((units, notes, HARM + 1) + both, f32),
            vmem((units, bands, PAIR, HARM + 2) + tile, jnp.int16),
            vmem((per, bands, HARM + 2) + tile, jnp.int16),
            vmem((bands + 1,) + tile, f32),
            vmem((1, width), f32),
            vmem((dates * pixes, 1, width), f32),
            dma,
            dma((dates,)),
            dma((dates,)),
            dma((units, bands + 1, dates)),
            dma((units, bands + 1, dates)),
            dma((units, merged + 1)),
            dma((units, merged + 1, 2)),
            dma((units,)),
            dma((units, notes)),
            dma((units, notes)),
            dma((units, bands, PAIR)),
            dma((per, bands)),
            dma((per, bands)),
            dma((per, bands)),
            dma((dates, pixes)),
            dma((dates * pixes,)),
        ],
        compiler_params=pltpu.CompilerParams(
            collective_id=0, has_side_effects=True, vmem_limit_bytes=60000000
        ),
    )(stack, quality, days)
    whole = pl.BlockSpec(memory_space=pltpu.VMEM)
    there = pl.BlockSpec(memory_space=pl.ANY)
    coef_shape = (bands, HARM, block, width * per)
    score_shape = (bands, block, width * per)
    return pl.pallas_call(
        finish,
        out_shape=(
            jax.ShapeDtypeStruct(coef_shape, f32),
            jax.ShapeDtypeStruct(score_shape, f32),
        ),
        in_specs=[whole, whole],
        out_specs=(there, there),
        scratch_shapes=[vmem(coef_shape, f32), vmem(score_shape, f32), dma((bands,)), dma],
        compiler_params=pltpu.CompilerParams(vmem_limit_bytes=20000000),
    )(fin, tot)


def solution(mesh):
    return jax.shard_map(
        functools.partial(local, mesh),
        mesh=mesh,
        in_specs=(P("date", None, None, "pix"), P("date", None, "pix"), P("date")),
        out_specs=(P(None, None, "pix", "date"), P(None, "pix", "date")),
        check_vma=False,
    )
```

```python
import functools

import jax
import jax.numpy as jnp
from jax import lax
from jax.experimental import pallas as pl
from jax.experimental.pallas import tpu as pltpu
from jax.sharding import PartitionSpec as P

RIDGE_TERM = 1.0
HARM = 8
PAIR = 2
LAG = 4
DIRECT = 1
MERGED = 6
REST_AT = 5
AHEAD = 1
BEHIND = 4
GRAM_AT = 2
LIMIT = 32767.0
LEVELS = 0x346C

MESH = pl.DeviceIdType.MESH
PAIR_LIST = [(first, second) for first in range(HARM) for second in range(first + 1)]
PAIR_AT = {pair: number for number, pair in enumerate(PAIR_LIST)}


def design_lanes(days):
    rows = [jnp.full((1, 128), day, jnp.int32) for day in days]
    moment_t = jnp.concatenate(rows, 0).astype(jnp.float32)
    lane = lax.broadcasted_iota(jnp.int32, moment_t.shape, 1)
    rate = jnp.where(
        lane < 4, 2.0 * jnp.pi, jnp.where(lane < 6, 4.0 * jnp.pi, 6.0 * jnp.pi))
    phase = rate * moment_t / 365.25
    wave = jnp.where(jnp.bitwise_and(lane, 1) == 0, jnp.cos(phase), jnp.sin(phase))
    linear = (moment_t - 512.0) / 512.0
    return jnp.where(lane == 0, 1.0, jnp.where(lane == 1, linear, wave))


def kernel(dims, stack, quality, days, fin, tot_ref,
           des_in, qbuf, code, raw, side, dall, bdes, wbuf, wside, gbuf, lbuf, lside,
           wsum_ref, note_out, note_in, res, rel, ssum, part, part_all,
           q_sem, des_send, des_recv, raw_send, raw_recv, side_send, side_recv,
           next_send, note_send, note_recv, hop_send, rel_recv, fin_send, fin_recv,
           part_send, part_recv):
    dates, pixes, times, bands, block = dims
    per = pixes // dates
    units = per // PAIR
    tall = PAIR * block
    s = lax.axis_index("date")
    q = lax.axis_index("pix")
    total = dates * times
    place = lax.rem(q, per)
    home = q // per
    merged = merged_bands(dates, bands)
    along = 1 + lax.rem(q, 2)
    across = 3 - along

    def peer_of(k):
        if dates & (dates - 1):
            return lax.rem(s + k, dates)
        return jnp.bitwise_xor(s, k)

    def group(sd):
        flip = lax.rem(q, 2)
        if dates & (dates - 1):
            return lax.rem(home + flip * (dates // 2) + 2 * dates - sd, dates)
        return jnp.bitwise_xor(jnp.bitwise_xor(home, sd), flip * (dates - 1))

    def far_of(r):
        flip = lax.rem(r, 2)
        if dates & (dates - 1):
            return lax.rem(home + s + dates - flip * (dates // 2), dates)
        return jnp.bitwise_xor(jnp.bitwise_xor(home, s), flip * (dates - 1))

    mine = group(s)

    barrier = pltpu.get_barrier_semaphore()
    others = [(k, kk) for k in range(dates) for kk in range(pixes) if k or kk]
    for k, kk in others:
        pl.semaphore_signal(barrier, inc=1, device_id=(peer_of(k), lax.rem(q + kk, pixes)),
                            device_id_type=MESH)

    q_copy = pltpu.make_async_copy(quality, qbuf, q_sem)
    q_copy.start()

    def rows_of(g, u):
        first = (g * units + u) * tall
        return pl.ds(pl.multiple_of(first, tall), tall)

    def mine_at(sd):
        return pl.ds(pl.multiple_of(sd * times, times), times)

    for u in range(units):
        for b in range(bands):
            pltpu.make_async_copy(
                stack.at[:, b, rows_of(mine, u), :], raw.at[u, b, mine_at(s)],
                raw_recv.at[u, b, s]).start()
            if b < merged:
                pltpu.make_async_copy(
                    stack.at[:, b, rows_of(group(peer_of(along)), u), :],
                    side.at[u, b, pl.ds(0, times)], side_recv.at[u, b, 0]).start()

    des_in[...] = design_lanes([days[r] for r in range(times)])
    q_copy.wait()
    for g in range(dates):
        for u in range(units):
            first = (g * units + u) * tall
            bits = qbuf[:, first:first + tall, :]
            digit = jnp.bitwise_and(jnp.right_shift(bits, 6), 12)
            value = jnp.bitwise_and(jnp.right_shift(jnp.full_like(bits, LEVELS), digit), 15)
            value = jnp.where(jnp.bitwise_and(bits, 8) == 0, value, 0)
            code[g, u] = value.astype(jnp.float32).astype(jnp.bfloat16)

    pl.semaphore_wait(barrier, len(others))

    def des_copy(k):
        return pltpu.make_async_remote_copy(
            des_in, dall.at[s], des_send.at[k], des_recv.at[s],
            device_id=(peer_of(k), q), device_id_type=MESH)

    def values_of(u, b, k):
        return stack.at[:, b, rows_of(group(peer_of(k)), u), :]

    def codes_of(u, k):
        return code.at[group(peer_of(k)), u]

    def raw_copy(src, u, b, k, slot):
        return pltpu.make_async_remote_copy(
            src, raw.at[u, b, mine_at(s)], raw_send.at[u, b, slot], raw_recv.at[u, b, s],
            device_id=(peer_of(k), q), device_id_type=MESH)

    def side_copy(src, u, b):
        return pltpu.make_async_remote_copy(
            src, side.at[u, b, pl.ds(times, times)], side_send.at[u, b], side_recv.at[u, b, 1],
            device_id=(peer_of(across), q), device_id_type=MESH)

    def next_copy(u):
        first = peer_of(across)
        return pltpu.make_async_remote_copy(
            side.at[u, merged, pl.ds(times, times)], raw.at[u, bands, mine_at(first)],
            next_send.at[u], raw_recv.at[u, bands, first],
            device_id=(peer_of(along), q), device_id_type=MESH)

    def note_copy(u, b):
        return pltpu.make_async_remote_copy(
            note_out.at[u, b], note_in.at[u, b], note_send.at[u, b], note_recv.at[u, b],
            device_id=(peer_of(along), q), device_id_type=MESH)

    order = list(range(dates - 1, 0, -1))

    def code_copies(u):
        if not merged:
            return [raw_copy(codes_of(u, k), u, bands, k, k) for k in order]
        return [side_copy(codes_of(u, dates - 1), u, merged),
                raw_copy(codes_of(u, across), u, bands, across, 1),
                raw_copy(codes_of(u, along), u, bands, along, 2)]

    def merged_copies(u, b):
        return [lambda: side_copy(values_of(u, b, dates - 1), u, b),
                lambda: raw_copy(values_of(u, b, across), u, b, across, 1)]

    def rest_copies(u, b):
        return [raw_copy(values_of(u, b, k), u, b, k, k) for k in order]

    for k in order:
        des_copy(k).start()
    for u in range(units):
        for c in code_copies(u):
            c.start()
        for b in range(merged + AHEAD):
            if b < merged:
                merged_copies(u, b)[0]().start()
            if b >= AHEAD:
                merged_copies(u, b - AHEAD)[1]().start()
        if not merged:
            for b in range(bands):
                for c in rest_copies(u, b):
                    c.start()
    for u in range(units):
        pltpu.make_async_copy(
            code.at[mine, u], raw.at[u, bands, mine_at(s)],
            raw_recv.at[u, bands, s]).start()
        if merged:
            pltpu.make_async_copy(
                code.at[group(peer_of(along)), u], side.at[u, merged, pl.ds(0, times)],
                side_recv.at[u, merged, 0]).start()

    def raw_wait(u, b, sd):
        there = raw.at[u, b, mine_at(sd)]
        pltpu.make_async_copy(there, there, raw_recv.at[u, b, sd]).wait()

    dall[s] = des_in[...]

    zero = jnp.zeros((PAIR, block, 128), jnp.float32)
    zero_one = jnp.zeros((block, 128), jnp.float32)
    for b in range(bands + 1):
        ssum[b] = zero_one

    def side_wait(u, b, slot):
        there = side.at[u, b, pl.ds(pl.multiple_of(slot * times, times), times)]
        pltpu.make_async_copy(there, there, side_recv.at[u, b, slot]).wait()

    def spread(k, wait):
        sd = peer_of(k)
        if wait:
            pltpu.make_async_copy(dall.at[sd], dall.at[sd], des_recv.at[sd]).wait()

        rows = dall[sd]
        for i in range(HARM):
            bdes[i, mine_at(sd), :] = jnp.broadcast_to(rows[:, i:i + 1], rows.shape)

    def design(t, i):
        return jnp.broadcast_to(bdes[i, pl.ds(t, 1), :], (block, 128))

    def pair_of(value):
        return value.astype(jnp.float32).reshape(PAIR, block, 128)

    def by_source(count, source_of, wait, body, carry, unroll):
        def source(n, carry):
            sd = source_of(n)
            wait(n, sd)
            return lax.fori_loop(
                0, times, lambda r, c: body(sd * times + r, n * times + r, c), carry,
                unroll=unroll)

        return lax.fori_loop(0, count, source, carry)

    every = (dates, peer_of)
    near = (2, lambda n: peer_of(n * across)) if merged else every
    far = (2, lambda n: peer_of(along + n * (dates - 1 - along)))

    def gram_over(sources, wait, code_at, weight_at, weight_to, out):
        def body(jj):
            def step(t, place_t, carry):
                if jj == 0:
                    both = pair_of(code_at(t, place_t)) * (1.0 / 12.0)
                    weight_to(t, place_t, both)
                    w = both[0]
                else:
                    w = weight_at(t, place_t, jj)
                d = [design(t, i) for i in range(HARM)]
                wd = [w] + [w * d[i] for i in range(1, HARM)]
                return tuple(
                    carry[n] + (wd[first] if second == 0 else wd[first] * d[second])
                    for n, (first, second) in enumerate(PAIR_LIST))
            return step

        start = (zero_one,) * len(PAIR_LIST)
        for jj in range(PAIR):
            gram = by_source(
                *sources, wait if jj == 0 else lambda n, sd: None, body(jj), start, 2)
            for n in range(len(PAIR_LIST)):
                out[n, jj] = gram[n]

    def factor(gram, out):
        lower = {}
        for first in range(HARM):
            for second in range(first + 1):
                value = gram[PAIR_AT[first, second]]
                if first == second:
                    value = value + RIDGE_TERM
                for inner in range(second):
                    value = value - lower[first, inner] * lower[second, inner]
                if first == second:
                    lower[first, first] = lax.rsqrt(value)
                else:
                    lower[first, second] = value * lower[second, second]
                out[PAIR_AT[first, second]] = lower[first, second]

    def solve(moment, lref):
        low = lambda first, second: lref[PAIR_AT[first, second]]
        forward = []
        for first in range(HARM):
            value = moment[first]
            for inner in range(first):
                value = value - low(first, inner) * forward[inner]
            forward.append(value * low(first, first))
        back = [None] * HARM
        for first in range(HARM - 1, -1, -1):
            value = forward[first]
            for inner in range(HARM - 1, first, -1):
                value = value - low(inner, first) * back[inner]
            back[first] = value * low(first, first)
        return back

    def moment_over(sources, wait, value_at, weight_at):
        def body(t, place_t, carry):
            wy = weight_at(t, place_t) * pair_of(value_at(t, place_t))
            return tuple(
                carry[i] + (wy if i == 0 else design(t, i) * wy) for i in range(HARM))

        return by_source(*sources, wait, body, (zero,) * HARM, 8)

    def residual_over(sources, back, value_at, weight_at):
        def body(t, place_t, ssr):
            terms = [back[0]] + [design(t, i) * back[i] for i in range(1, HARM)]
            while len(terms) > 1:
                terms = [terms[i] + terms[i + 1] for i in range(0, len(terms), 2)]
            diff = pair_of(value_at(t, place_t)) - terms[0]
            return ssr + weight_at(t, place_t) * diff * diff

        return by_source(*sources, lambda n, sd: None, body, zero, 8)

    def side_gram(u):
        def wait(n, sd):
            side_wait(u, merged, n)

            @pl.when(n == 1)
            def _():
                next_copy(u).start()

        def keep(t, place_t, both):
            wside[place_t] = both

        gram_over(near, wait, lambda t, place_t: side[u, merged, place_t],
                  lambda t, place_t, jj: wside[place_t, jj], keep, lside)
        factor([lside[n] for n in range(len(PAIR_LIST))], lside)

    def side_step(u, b):
        value_at = lambda t, place_t: side[u, b, place_t]
        weight_at = lambda t, place_t: wside[place_t]
        moment = moment_over(near, lambda n, sd: side_wait(u, b, n), value_at, weight_at)
        back = solve(moment, lside)
        for i in range(HARM):
            note_out[u, b, i] = back[i]
        note_out[u, b, HARM] = residual_over(near, back, value_at, weight_at)
        note_copy(u, b).start()

    def own_gram(u):
        def keep(t, place_t, both):
            wbuf[t] = both

        def over(sources, out):
            gram_over(sources, lambda n, sd: raw_wait(u, bands, sd),
                      lambda t, place_t: raw[u, bands, t],
                      lambda t, place_t, jj: wbuf[t, jj], keep, out)

        over(near, lbuf)
        if merged:
            over(far, gbuf)
            gram = [lbuf[n] + gbuf[n] for n in range(len(PAIR_LIST))]
        else:
            gram = [lbuf[n] for n in range(len(PAIR_LIST))]
        wsum_ref[...] = 1.0 / (gram[0] + 1.0)
        ssum[bands] = ssum[bands] + jnp.sum(gram[0], 0)
        factor(gram, lbuf)

    def far_gram_times(vector):
        rows = []
        for first in range(HARM):
            row = None
            for second in range(HARM):
                pair = (max(first, second), min(first, second))
                term = gbuf[PAIR_AT[pair]] * vector[second]
                row = term if row is None else row + term
            rows.append(row)
        return rows

    def hop(u, b, start):
        for jj in range(PAIR):
            p = mine * per + PAIR * u + jj

            def act(dst, sem):
                @pl.when(p != q)
                def _():
                    c = pltpu.make_async_remote_copy(
                        res.at[u, b, jj], dst, hop_send.at[u, b, jj], sem,
                        device_id=(s, p), device_id_type=MESH)
                    c.start() if start else c.wait_send()

                if start:
                    @pl.when(p == q)
                    def _():
                        pltpu.make_async_copy(res.at[u, b, jj], dst, sem).start()

            @pl.when(home == s)
            def _():
                act(fin.at[place, b], fin_recv.at[place, b])

            late = u * bands + b >= units * bands - DIRECT

            @pl.when(jnp.logical_and(home != s, jnp.logical_not(late)))
            def _():
                act(rel.at[place, b], rel_recv.at[place, b])

            @pl.when(jnp.logical_and(home != s, late))
            def _():
                c = pltpu.make_async_remote_copy(
                    res.at[u, b, jj], fin.at[place, b], hop_send.at[u, b, jj],
                    fin_recv.at[place, b], device_id=(home, p), device_id_type=MESH)
                c.start() if start else c.wait_send()

    def band_step(u, b, with_note):
        value_at = lambda t, place_t: raw[u, b, t]
        weight_at = lambda t, place_t: wbuf[t]
        sources = near if with_note else every
        moment = moment_over(
            sources, lambda n, sd: raw_wait(u, b, sd), value_at, weight_at)
        if with_note:
            pltpu.make_async_copy(note_in.at[u, b], note_in.at[u, b], note_recv.at[u, b]).wait()
            fit = [note_in[u, b, i] for i in range(HARM)]
            rows = far_gram_times(fit)
            moment = [moment[i] + (rows[i] + fit[i]) for i in range(HARM)]
        back = solve(moment, lbuf)
        ssr = residual_over(sources, back, value_at, weight_at)
        if with_note:
            fit = [note_in[u, b, i] for i in range(HARM)]
            shift = [back[i] - fit[i] for i in range(HARM)]
            rows = far_gram_times(shift)
            extra = note_in[u, b, HARM]
            for i in range(HARM):
                extra = extra + shift[i] * (rows[i] - 2.0 * fit[i])
            ssr = jnp.maximum(ssr + extra, 0.0)
        ratio = jnp.sqrt(ssr * wsum_ref[...])
        peak = ratio
        for i in range(HARM):
            peak = jnp.maximum(peak, jnp.abs(back[i]))
        level = jnp.ceil(jnp.log2(jnp.maximum(peak, 1e-36)) + 0.01)
        inverse = jnp.exp2(-level)
        scale = inverse * LIMIT
        for i in range(HARM):
            put(res, u, b, i, jnp.floor(jnp.clip(back[i] * scale, -LIMIT, LIMIT) + 0.5))
        root = jnp.sqrt(jnp.sqrt(jnp.minimum(ratio * inverse, 1.0)))
        put(res, u, b, HARM, jnp.floor(root * LIMIT + 0.5))
        put(res, u, b, HARM + 1, level)
        ssum[b] = ssum[b] + jnp.sum(ssr, 0)
        hop(u, b, True)

    def pass_on(r, b, start):
        far = far_of(r)

        @pl.when(far != s)
        def _():
            c = pltpu.make_async_remote_copy(
                rel.at[r, b], fin.at[r, b], fin_send.at[r, b], fin_recv.at[r, b],
                device_id=(far, q), device_id_type=MESH)
            if start:
                pltpu.make_async_copy(rel.at[r, b], rel.at[r, b], rel_recv.at[r, b]).wait()
                c.start()
            else:
                c.wait_send()

    def relay(n):
        b = lax.rem(n, bands)

        @pl.when(n // bands == place // PAIR)
        def _():
            for r in range(per):
                pass_on(r, b, True)

    def rest_at(u, act):
        for b in range(merged, bands):
            for c in rest_copies(u, b):
                act(c)

    if merged:
        spread(0, False)
        spread(across, True)
    else:
        for k in range(dates):
            spread(k, k > 0)

    behind = BEHIND if merged else 1
    gram_at = GRAM_AT if merged else 0
    steps = bands + behind

    @pl.loop(0, units * steps)
    def _(n):
        u = n // steps
        step = lax.rem(n, steps)
        if merged:
            @pl.when(step == 0)
            def _():
                side_gram(u)

            @pl.when(step < merged)
            def _():
                side_step(u, step)

            @pl.when(n == 0)
            def _():
                spread(along, True)
                spread(dates - 1, True)

            @pl.when(step == REST_AT)
            def _():
                rest_at(u, lambda c: c.start())

        @pl.when(step == gram_at)
        def _():
            own_gram(u)

        b = step - behind
        if merged:
            @pl.when(jnp.logical_and(b >= 0, b < merged))
            def _():
                band_step(u, b, True)

        if merged < bands:
            @pl.when(b >= merged)
            def _():
                band_step(u, b, False)

        done = u * bands + b

        @pl.when(jnp.logical_and(b >= 0, done >= LAG))
        def _():
            relay(done - LAG)

    sums = jnp.concatenate(
        [jnp.sum(ssum[b], 0, keepdims=True) for b in range(bands + 1)], 0)
    sums = jnp.broadcast_to(jnp.sum(sums, 1, keepdims=True), sums.shape)
    lane = lax.broadcasted_iota(jnp.int32, sums.shape, 1)
    row = lax.broadcasted_iota(jnp.int32, sums.shape, 0)
    part[...] = jnp.sum(jnp.where(lane == row, sums, 0.0), 0, keepdims=True)
    here = s * pixes + q

    def part_copy(k, kk):
        return pltpu.make_async_remote_copy(
            part, part_all.at[here], part_send.at[k, kk], part_recv.at[here],
            device_id=(peer_of(k), lax.rem(q + kk, pixes)), device_id_type=MESH)

    for k, kk in others:
        part_copy(k, kk).start()
    part_all[here] = part[...]
    for n in range(LAG, DIRECT, -1):
        relay(units * bands - n)

    @pl.loop(0, bands)
    def _(b):
        for r in range(per):
            pltpu.make_async_copy(fin.at[r, b], fin.at[r, b], fin_recv.at[r, b]).wait()

    for k, kk in others:
        there = peer_of(k) * pixes + lax.rem(q + kk, pixes)
        pltpu.make_async_copy(part_all.at[there], part_all.at[there], part_recv.at[there]).wait()
    terms = [part_all[n] for n in range(dates * pixes)]
    while len(terms) > 1:
        terms = [sum(terms[i:i + 2]) for i in range(0, len(terms), 2)]
    tot_ref[...] = terms[0]

    for k in range(1, dates):
        des_copy(k).wait_send()
    for k, kk in others:
        part_copy(k, kk).wait_send()

    @pl.loop(0, units)
    def _(u):
        for c in code_copies(u):
            c.wait_send()
        if merged:
            next_copy(u).wait_send()

            @pl.loop(0, merged)
            def _(b):
                for c in merged_copies(u, b):
                    c().wait_send()
                note_copy(u, b).wait_send()
            rest_at(u, lambda c: c.wait_send())
        else:
            @pl.loop(0, bands)
            def _(b):
                for c in rest_copies(u, b):
                    c.wait_send()

        @pl.loop(0, bands)
        def _(b):
            hop(u, b, False)

    @pl.loop(0, bands)
    def _(b):
        @pl.when((place // PAIR) * bands + b < units * bands - DIRECT)
        def _():
            for r in range(per):
                pass_on(r, b, False)


def merged_bands(dates, bands):
    return min(MERGED, bands - 1) if dates == 4 else 0


def put(res, u, b, i, value):
    whole = value.astype(jnp.int32)
    for jj in range(PAIR):
        res[u, b, jj, i] = whole[jj].astype(jnp.int16)


def finish(fin, tot_ref, coef, score, coef_buf, score_buf, coef_sem, score_sem):
    per, bands = fin.shape[:2]
    copies = []
    tot = tot_ref[...]
    for b in range(bands):
        sigma = jnp.sqrt(tot[:, b:b + 1] / tot[:, bands:bands + 1])
        scale = jnp.broadcast_to(1.0 / sigma, fin.shape[3:])
        for r in range(per):
            cols = slice(r * 128, (r + 1) * 128)
            number = lambda i: fin[r, b, i].astype(jnp.int32).astype(jnp.float32)
            unit = jnp.exp2(number(HARM + 1))
            step = unit * (1.0 / LIMIT)
            for i in range(HARM):
                coef_buf[b, i, :, cols] = number(i) * step
            root = number(HARM) * (1.0 / LIMIT)
            root = root * root
            score_buf[b, :, cols] = root * root * (unit * scale)
        copies.append(pltpu.make_async_copy(coef_buf.at[b], coef.at[b], coef_sem.at[b]))
        copies[-1].start()
    copies.append(pltpu.make_async_copy(score_buf, score, score_sem))
    copies[-1].start()
    for c in copies:
        c.wait()


def local(mesh, stack, quality, days):
    dates, pixes = mesh.shape["date"], mesh.shape["pix"]
    times, bands, rows, width = stack.shape
    block = rows // pixes
    per = pixes // dates
    units = per // PAIR
    total = dates * times
    dims = (dates, pixes, times, bands, block)
    merged = merged_bands(dates, bands)
    notes = max(merged, 1)
    tile = (block, width)
    both = (PAIR,) + tile
    tall = (PAIR * block, width)
    vmem, dma = pltpu.VMEM, pltpu.SemaphoreType.DMA
    f32, bf16 = jnp.float32, jnp.bfloat16
    fin, tot = pl.pallas_call(
        functools.partial(kernel, dims),
        out_shape=(
            vmem((per, bands, HARM + 2) + tile, jnp.int16),
            vmem((1, width), f32),
        ),
        in_specs=[
            pl.BlockSpec(memory_space=pl.ANY),
            pl.BlockSpec(memory_space=pl.ANY),
            pl.BlockSpec(memory_space=pltpu.SMEM),
        ],
        out_specs=(
            pl.BlockSpec(memory_space=pltpu.VMEM),
            pl.BlockSpec(memory_space=pltpu.VMEM),
        ),
        scratch_shapes=[
            vmem((times, 128), f32),
            vmem((times, rows, width), jnp.int32),
            vmem((dates, units, times) + tall, bf16),
            vmem((units, bands + 1, total) + tall, bf16),
            vmem((units, merged + 1, 2 * times) + tall, bf16),
            vmem((dates, times, 128), f32),
            vmem((HARM, total, width), f32),
            vmem((total,) + both, f32),
            vmem((2 * times,) + both, f32),
            vmem((len(PAIR_LIST),) + both, f32),
            vmem((len(PAIR_LIST),) + both, f32),
            vmem((len(PAIR_LIST),) + both, f32),
            vmem(both, f32),
            vmem((units, notes, HARM + 1) + both, f32),
            vmem((units, notes, HARM + 1) + both, f32),
            vmem((units, bands, PAIR, HARM + 2) + tile, jnp.int16),
            vmem((per, bands, HARM + 2) + tile, jnp.int16),
            vmem((bands + 1,) + tile, f32),
            vmem((1, width), f32),
            vmem((dates * pixes, 1, width), f32),
            dma,
            dma((dates,)),
            dma((dates,)),
            dma((units, bands + 1, dates)),
            dma((units, bands + 1, dates)),
            dma((units, merged + 1)),
            dma((units, merged + 1, 2)),
            dma((units,)),
            dma((units, notes)),
            dma((units, notes)),
            dma((units, bands, PAIR)),
            dma((per, bands)),
            dma((per, bands)),
            dma((per, bands)),
            dma((dates, pixes)),
            dma((dates * pixes,)),
        ],
        compiler_params=pltpu.CompilerParams(
            collective_id=0, has_side_effects=True, vmem_limit_bytes=60000000
        ),
    )(stack, quality, days)
    whole = pl.BlockSpec(memory_space=pltpu.VMEM)
    there = pl.BlockSpec(memory_space=pl.ANY)
    coef_shape = (bands, HARM, block, width * per)
    score_shape = (bands, block, width * per)
    return pl.pallas_call(
        finish,
        out_shape=(
            jax.ShapeDtypeStruct(coef_shape, f32),
            jax.ShapeDtypeStruct(score_shape, f32),
        ),
        in_specs=[whole, whole],
        out_specs=(there, there),
        scratch_shapes=[vmem(coef_shape, f32), vmem(score_shape, f32), dma((bands,)), dma],
        compiler_params=pltpu.CompilerParams(vmem_limit_bytes=20000000),
    )(fin, tot)


def solution(mesh):
    return jax.shard_map(
        functools.partial(local, mesh),
        mesh=mesh,
        in_specs=(P("date", None, None, "pix"), P("date", None, "pix"), P("date")),
        out_specs=(P(None, None, "pix", "date"), P(None, "pix", "date")),
        check_vma=False,
    )
```

```python
import functools

import jax
import jax.numpy as jnp
from jax import lax
from jax.experimental import pallas as pl
from jax.experimental.pallas import tpu as pltpu
from jax.sharding import PartitionSpec as P

RIDGE_TERM = 1.0
HARM = 8
PAIR = 2
LAG = 4
DIRECT = 1
MERGED = 6
REST_AT = 5
AHEAD = 1
BEHIND = 4
GRAM_AT = 2
LIMIT = 32767.0
LEVELS = 0x346C

MESH = pl.DeviceIdType.MESH
PAIR_LIST = [(first, second) for first in range(HARM) for second in range(first + 1)]
PAIR_AT = {pair: number for number, pair in enumerate(PAIR_LIST)}


def design_lanes(days):
    rows = [jnp.full((1, 128), day, jnp.int32) for day in days]
    moment_t = jnp.concatenate(rows, 0).astype(jnp.float32)
    lane = lax.broadcasted_iota(jnp.int32, moment_t.shape, 1)
    rate = jnp.where(
        lane < 4, 2.0 * jnp.pi, jnp.where(lane < 6, 4.0 * jnp.pi, 6.0 * jnp.pi))
    phase = rate * moment_t / 365.25
    wave = jnp.where(jnp.bitwise_and(lane, 1) == 0, jnp.cos(phase), jnp.sin(phase))
    linear = (moment_t - 512.0) / 512.0
    return jnp.where(lane == 0, 1.0, jnp.where(lane == 1, linear, wave))


def kernel(dims, stack, quality, days, fin, tot_ref,
           des_in, qbuf, code, raw, side, dall, bdes, wbuf, wside, gbuf, lbuf, lside,
           wsum_ref, note_out, note_in, res, rel, ssum, part, part_all,
           q_sem, des_send, des_recv, raw_send, raw_recv, side_send, side_recv,
           next_send, note_send, note_recv, hop_send, rel_recv, fin_send, fin_recv,
           part_send, part_recv):
    dates, pixes, times, bands, block = dims
    per = pixes // dates
    units = per // PAIR
    tall = PAIR * block
    s = lax.axis_index("date")
    q = lax.axis_index("pix")
    total = dates * times
    place = lax.rem(q, per)
    home = q // per
    merged = merged_bands(dates, bands)
    along = 1 + lax.rem(q, 2)
    across = 3 - along

    def peer_of(k):
        if dates & (dates - 1):
            return lax.rem(s + k, dates)
        return jnp.bitwise_xor(s, k)

    def group(sd):
        flip = lax.rem(q, 2)
        if dates & (dates - 1):
            return lax.rem(home + flip * (dates // 2) + 2 * dates - sd, dates)
        return jnp.bitwise_xor(jnp.bitwise_xor(home, sd), flip * (dates - 1))

    def far_of(r):
        flip = lax.rem(r, 2)
        if dates & (dates - 1):
            return lax.rem(home + s + dates - flip * (dates // 2), dates)
        return jnp.bitwise_xor(jnp.bitwise_xor(home, s), flip * (dates - 1))

    mine = group(s)

    barrier = pltpu.get_barrier_semaphore()
    others = [(k, kk) for k in range(dates) for kk in range(pixes) if k or kk]
    for k, kk in others:
        pl.semaphore_signal(barrier, inc=1, device_id=(peer_of(k), lax.rem(q + kk, pixes)),
                            device_id_type=MESH)

    q_copy = pltpu.make_async_copy(quality, qbuf, q_sem)
    q_copy.start()

    def rows_of(g, u):
        first = (g * units + u) * tall
        return pl.ds(pl.multiple_of(first, tall), tall)

    def mine_at(sd):
        return pl.ds(pl.multiple_of(sd * times, times), times)

    for u in range(units):
        for b in range(bands):
            pltpu.make_async_copy(
                stack.at[:, b, rows_of(mine, u), :], raw.at[u, b, mine_at(s)],
                raw_recv.at[u, b, s]).start()
            if b < merged:
                pltpu.make_async_copy(
                    stack.at[:, b, rows_of(group(peer_of(along)), u), :],
                    side.at[u, b, pl.ds(0, times)], side_recv.at[u, b, 0]).start()

    des_in[...] = design_lanes([days[r] for r in range(times)])
    q_copy.wait()
    for g in range(dates):
        for u in range(units):
            first = (g * units + u) * tall
            bits = qbuf[:, first:first + tall, :]
            digit = jnp.bitwise_and(jnp.right_shift(bits, 6), 12)
            value = jnp.bitwise_and(jnp.right_shift(jnp.full_like(bits, LEVELS), digit), 15)
            value = jnp.where(jnp.bitwise_and(bits, 8) == 0, value, 0)
            code[g, u] = value.astype(jnp.float32).astype(jnp.bfloat16)

    pl.semaphore_wait(barrier, len(others))

    def des_copy(k):
        return pltpu.make_async_remote_copy(
            des_in, dall.at[s], des_send.at[k], des_recv.at[s],
            device_id=(peer_of(k), q), device_id_type=MESH)

    def values_of(u, b, k):
        return stack.at[:, b, rows_of(group(peer_of(k)), u), :]

    def codes_of(u, k):
        return code.at[group(peer_of(k)), u]

    def raw_copy(src, u, b, k, slot):
        return pltpu.make_async_remote_copy(
            src, raw.at[u, b, mine_at(s)], raw_send.at[u, b, slot], raw_recv.at[u, b, s],
            device_id=(peer_of(k), q), device_id_type=MESH)

    def side_copy(src, u, b):
        return pltpu.make_async_remote_copy(
            src, side.at[u, b, pl.ds(times, times)], side_send.at[u, b], side_recv.at[u, b, 1],
            device_id=(peer_of(across), q), device_id_type=MESH)

    def next_copy(u):
        first = peer_of(across)
        return pltpu.make_async_remote_copy(
            side.at[u, merged, pl.ds(times, times)], raw.at[u, bands, mine_at(first)],
            next_send.at[u], raw_recv.at[u, bands, first],
            device_id=(peer_of(along), q), device_id_type=MESH)

    def note_copy(u, b):
        return pltpu.make_async_remote_copy(
            note_out.at[u, b], note_in.at[u, b], note_send.at[u, b], note_recv.at[u, b],
            device_id=(peer_of(along), q), device_id_type=MESH)

    order = list(range(dates - 1, 0, -1))

    def code_copies(u):
        if not merged:
            return [raw_copy(codes_of(u, k), u, bands, k, k) for k in order]
        return [side_copy(codes_of(u, dates - 1), u, merged),
                raw_copy(codes_of(u, across), u, bands, across, 1),
                raw_copy(codes_of(u, along), u, bands, along, 2)]

    def merged_copies(u, b):
        return [lambda: side_copy(values_of(u, b, dates - 1), u, b),
                lambda: raw_copy(values_of(u, b, across), u, b, across, 1)]

    def rest_copies(u, b):
        return [raw_copy(values_of(u, b, k), u, b, k, k) for k in order]

    for k in order:
        des_copy(k).start()
    for u in range(units):
        for c in code_copies(u):
            c.start()
        for b in range(merged + AHEAD):
            if b < merged:
                merged_copies(u, b)[0]().start()
            if b >= AHEAD:
                merged_copies(u, b - AHEAD)[1]().start()
        if not merged:
            for b in range(bands):
                for c in rest_copies(u, b):
                    c.start()
    for u in range(units):
        pltpu.make_async_copy(
            code.at[mine, u], raw.at[u, bands, mine_at(s)],
            raw_recv.at[u, bands, s]).start()
        if merged:
            pltpu.make_async_copy(
                code.at[group(peer_of(along)), u], side.at[u, merged, pl.ds(0, times)],
                side_recv.at[u, merged, 0]).start()

    def raw_wait(u, b, sd):
        there = raw.at[u, b, mine_at(sd)]
        pltpu.make_async_copy(there, there, raw_recv.at[u, b, sd]).wait()

    dall[s] = des_in[...]

    zero = jnp.zeros((PAIR, block, 128), jnp.float32)
    zero_one = jnp.zeros((block, 128), jnp.float32)
    for b in range(bands + 1):
        ssum[b] = zero_one

    def side_wait(u, b, slot):
        there = side.at[u, b, pl.ds(pl.multiple_of(slot * times, times), times)]
        pltpu.make_async_copy(there, there, side_recv.at[u, b, slot]).wait()

    def spread(k, wait):
        sd = peer_of(k)
        if wait:
            pltpu.make_async_copy(dall.at[sd], dall.at[sd], des_recv.at[sd]).wait()

        rows = dall[sd]
        for i in range(HARM):
            bdes[i, mine_at(sd), :] = jnp.broadcast_to(rows[:, i:i + 1], rows.shape)

    def design(t, i):
        return jnp.broadcast_to(bdes[i, pl.ds(t, 1), :], (block, 128))

    def pair_of(value):
        return value.astype(jnp.float32).reshape(PAIR, block, 128)

    def by_source(count, source_of, wait, body, carry, unroll):
        def source(n, carry):
            sd = source_of(n)
            wait(n, sd)
            return lax.fori_loop(
                0, times, lambda r, c: body(sd * times + r, n * times + r, c), carry,
                unroll=unroll)

        return lax.fori_loop(0, count, source, carry)

    every = (dates, peer_of)
    near = (2, lambda n: peer_of(n * across)) if merged else every
    far = (2, lambda n: peer_of(along + n * (dates - 1 - along)))

    def gram_over(sources, wait, code_at, weight_at, weight_to, out):
        def body(jj):
            def step(t, place_t, carry):
                if jj == 0:
                    both = pair_of(code_at(t, place_t)) * (1.0 / 12.0)
                    weight_to(t, place_t, both)
                    w = both[0]
                else:
                    w = weight_at(t, place_t, jj)
                d = [design(t, i) for i in range(HARM)]
                wd = [w] + [w * d[i] for i in range(1, HARM)]
                return tuple(
                    carry[n] + (wd[first] if second == 0 else wd[first] * d[second])
                    for n, (first, second) in enumerate(PAIR_LIST))
            return step

        start = (zero_one,) * len(PAIR_LIST)
        for jj in range(PAIR):
            gram = by_source(
                *sources, wait if jj == 0 else lambda n, sd: None, body(jj), start, 2)
            for n in range(len(PAIR_LIST)):
                out[n, jj] = gram[n]

    def factor(gram, out):
        lower = {}
        for first in range(HARM):
            for second in range(first + 1):
                value = gram[PAIR_AT[first, second]]
                if first == second:
                    value = value + RIDGE_TERM
                for inner in range(second):
                    value = value - lower[first, inner] * lower[second, inner]
                if first == second:
                    lower[first, first] = lax.rsqrt(value)
                else:
                    lower[first, second] = value * lower[second, second]
                out[PAIR_AT[first, second]] = lower[first, second]

    def solve(moment, lref):
        low = lambda first, second: lref[PAIR_AT[first, second]]
        forward = []
        for first in range(HARM):
            value = moment[first]
            for inner in range(first):
                value = value - low(first, inner) * forward[inner]
            forward.append(value * low(first, first))
        back = [None] * HARM
        for first in range(HARM - 1, -1, -1):
            value = forward[first]
            for inner in range(HARM - 1, first, -1):
                value = value - low(inner, first) * back[inner]
            back[first] = value * low(first, first)
        return back

    def moment_over(sources, wait, value_at, weight_at):
        def body(t, place_t, carry):
            wy = weight_at(t, place_t) * pair_of(value_at(t, place_t))
            return tuple(
                carry[i] + (wy if i == 0 else design(t, i) * wy) for i in range(HARM))

        return by_source(*sources, wait, body, (zero,) * HARM, 8)

    def residual_over(sources, back, value_at, weight_at):
        def body(t, place_t, ssr):
            terms = [back[0]] + [design(t, i) * back[i] for i in range(1, HARM)]
            while len(terms) > 1:
                terms = [terms[i] + terms[i + 1] for i in range(0, len(terms), 2)]
            diff = pair_of(value_at(t, place_t)) - terms[0]
            return ssr + weight_at(t, place_t) * diff * diff

        return by_source(*sources, lambda n, sd: None, body, zero, 8)

    def side_gram(u):
        def wait(n, sd):
            side_wait(u, merged, n)

            @pl.when(n == 1)
            def _():
                next_copy(u).start()

        def keep(t, place_t, both):
            wside[place_t] = both

        gram_over(near, wait, lambda t, place_t: side[u, merged, place_t],
                  lambda t, place_t, jj: wside[place_t, jj], keep, lside)
        factor([lside[n] for n in range(len(PAIR_LIST))], lside)

    def side_step(u, b):
        value_at = lambda t, place_t: side[u, b, place_t]
        weight_at = lambda t, place_t: wside[place_t]
        moment = moment_over(near, lambda n, sd: side_wait(u, b, n), value_at, weight_at)
        back = solve(moment, lside)
        for i in range(HARM):
            note_out[u, b, i] = back[i]
        note_out[u, b, HARM] = residual_over(near, back, value_at, weight_at)
        note_copy(u, b).start()

    def own_gram(u):
        def keep(t, place_t, both):
            wbuf[t] = both

        def over(sources, out):
            gram_over(sources, lambda n, sd: raw_wait(u, bands, sd),
                      lambda t, place_t: raw[u, bands, t],
                      lambda t, place_t, jj: wbuf[t, jj], keep, out)

        over(near, lbuf)
        if merged:
            over(far, gbuf)
            gram = [lbuf[n] + gbuf[n] for n in range(len(PAIR_LIST))]
        else:
            gram = [lbuf[n] for n in range(len(PAIR_LIST))]
        wsum_ref[...] = 1.0 / (gram[0] + 1.0)
        ssum[bands] = ssum[bands] + jnp.sum(gram[0], 0)
        factor(gram, lbuf)

    def far_gram_times(vector):
        rows = []
        for first in range(HARM):
            row = None
            for second in range(HARM):
                pair = (max(first, second), min(first, second))
                term = gbuf[PAIR_AT[pair]] * vector[second]
                row = term if row is None else row + term
            rows.append(row)
        return rows

    def hop(u, b, start):
        for jj in range(PAIR):
            p = mine * per + PAIR * u + jj

            def act(dst, sem):
                @pl.when(p != q)
                def _():
                    c = pltpu.make_async_remote_copy(
                        res.at[u, b, jj], dst, hop_send.at[u, b, jj], sem,
                        device_id=(s, p), device_id_type=MESH)
                    c.start() if start else c.wait_send()

                if start:
                    @pl.when(p == q)
                    def _():
                        pltpu.make_async_copy(res.at[u, b, jj], dst, sem).start()

            @pl.when(home == s)
            def _():
                act(fin.at[place, b], fin_recv.at[place, b])

            late = u * bands + b >= units * bands - DIRECT

            @pl.when(jnp.logical_and(home != s, jnp.logical_not(late)))
            def _():
                act(rel.at[place, b], rel_recv.at[place, b])

            @pl.when(jnp.logical_and(home != s, late))
            def _():
                c = pltpu.make_async_remote_copy(
                    res.at[u, b, jj], fin.at[place, b], hop_send.at[u, b, jj],
                    fin_recv.at[place, b], device_id=(home, p), device_id_type=MESH)
                c.start() if start else c.wait_send()

    def band_step(u, b, with_note):
        value_at = lambda t, place_t: raw[u, b, t]
        weight_at = lambda t, place_t: wbuf[t]
        sources = near if with_note else every
        moment = moment_over(
            sources, lambda n, sd: raw_wait(u, b, sd), value_at, weight_at)
        if with_note:
            pltpu.make_async_copy(note_in.at[u, b], note_in.at[u, b], note_recv.at[u, b]).wait()
            fit = [note_in[u, b, i] for i in range(HARM)]
            rows = far_gram_times(fit)
            moment = [moment[i] + (rows[i] + fit[i]) for i in range(HARM)]
        back = solve(moment, lbuf)
        ssr = residual_over(sources, back, value_at, weight_at)
        if with_note:
            fit = [note_in[u, b, i] for i in range(HARM)]
            shift = [back[i] - fit[i] for i in range(HARM)]
            rows = far_gram_times(shift)
            extra = note_in[u, b, HARM]
            for i in range(HARM):
                extra = extra + shift[i] * (rows[i] - 2.0 * fit[i])
            ssr = jnp.maximum(ssr + extra, 0.0)
        ratio = jnp.sqrt(ssr * wsum_ref[...])
        peak = ratio
        for i in range(HARM):
            peak = jnp.maximum(peak, jnp.abs(back[i]))
        level = jnp.ceil(jnp.log2(jnp.maximum(peak, 1e-36)) + 0.01)
        inverse = jnp.exp2(-level)
        scale = inverse * LIMIT
        for i in range(HARM):
            put(res, u, b, i, jnp.floor(jnp.clip(back[i] * scale, -LIMIT, LIMIT) + 0.5))
        root = jnp.sqrt(jnp.sqrt(jnp.minimum(ratio * inverse, 1.0)))
        put(res, u, b, HARM, jnp.floor(root * LIMIT + 0.5))
        put(res, u, b, HARM + 1, level)
        ssum[b] = ssum[b] + jnp.sum(ssr, 0)
        hop(u, b, True)

    def pass_on(r, b, start):
        far = far_of(r)

        @pl.when(far != s)
        def _():
            c = pltpu.make_async_remote_copy(
                rel.at[r, b], fin.at[r, b], fin_send.at[r, b], fin_recv.at[r, b],
                device_id=(far, q), device_id_type=MESH)
            if start:
                pltpu.make_async_copy(rel.at[r, b], rel.at[r, b], rel_recv.at[r, b]).wait()
                c.start()
            else:
                c.wait_send()

    def relay(n):
        b = lax.rem(n, bands)

        @pl.when(n // bands == place // PAIR)
        def _():
            for r in range(per):
                pass_on(r, b, True)

    def rest_at(u, act):
        for b in range(merged, bands):
            for c in rest_copies(u, b):
                act(c)

    if merged:
        spread(0, False)
        spread(across, True)
    else:
        for k in range(dates):
            spread(k, k > 0)

    behind = BEHIND if merged else 1
    gram_at = GRAM_AT if merged else 0
    steps = bands + behind

    @pl.loop(0, units * steps)
    def _(n):
        u = n // steps
        step = lax.rem(n, steps)
        if merged:
            @pl.when(step == 0)
            def _():
                side_gram(u)

            @pl.when(step < merged)
            def _():
                side_step(u, step)

            @pl.when(n == 0)
            def _():
                spread(along, True)
                spread(dates - 1, True)

            @pl.when(step == REST_AT)
            def _():
                rest_at(u, lambda c: c.start())

        @pl.when(step == gram_at)
        def _():
            own_gram(u)

        b = step - behind
        if merged:
            @pl.when(jnp.logical_and(b >= 0, b < merged))
            def _():
                band_step(u, b, True)

        if merged < bands:
            @pl.when(b >= merged)
            def _():
                band_step(u, b, False)

        done = u * bands + b

        @pl.when(jnp.logical_and(b >= 0, done >= LAG))
        def _():
            relay(done - LAG)

    sums = jnp.concatenate(
        [jnp.sum(ssum[b], 0, keepdims=True) for b in range(bands + 1)], 0)
    sums = jnp.broadcast_to(jnp.sum(sums, 1, keepdims=True), sums.shape)
    lane = lax.broadcasted_iota(jnp.int32, sums.shape, 1)
    row = lax.broadcasted_iota(jnp.int32, sums.shape, 0)
    part[...] = jnp.sum(jnp.where(lane == row, sums, 0.0), 0, keepdims=True)
    here = s * pixes + q

    def part_copy(k, kk):
        return pltpu.make_async_remote_copy(
            part, part_all.at[here], part_send.at[k, kk], part_recv.at[here],
            device_id=(peer_of(k), lax.rem(q + kk, pixes)), device_id_type=MESH)

    for k, kk in reversed(others):
        part_copy(k, kk).start()
    part_all[here] = part[...]
    for n in range(LAG, DIRECT, -1):
        relay(units * bands - n)

    for k in range(1, dates):
        des_copy(k).wait_send()
    for k, kk in others:
        part_copy(k, kk).wait_send()

    @pl.loop(0, units)
    def _(u):
        for c in code_copies(u):
            c.wait_send()
        if merged:
            next_copy(u).wait_send()

            @pl.loop(0, merged)
            def _(b):
                for c in merged_copies(u, b):
                    c().wait_send()
                note_copy(u, b).wait_send()
            rest_at(u, lambda c: c.wait_send())
        else:
            @pl.loop(0, bands)
            def _(b):
                for c in rest_copies(u, b):
                    c.wait_send()

        @pl.loop(0, bands)
        def _(b):
            hop(u, b, False)

    @pl.loop(0, bands)
    def _(b):
        @pl.when((place // PAIR) * bands + b < units * bands - DIRECT)
        def _():
            for r in range(per):
                pass_on(r, b, False)

    @pl.loop(0, bands)
    def _(b):
        for r in range(per):
            pltpu.make_async_copy(fin.at[r, b], fin.at[r, b], fin_recv.at[r, b]).wait()

    for k, kk in others:
        there = peer_of(k) * pixes + lax.rem(q + kk, pixes)
        pltpu.make_async_copy(part_all.at[there], part_all.at[there], part_recv.at[there]).wait()
    terms = [part_all[n] for n in range(dates * pixes)]
    while len(terms) > 1:
        terms = [sum(terms[i:i + 2]) for i in range(0, len(terms), 2)]
    tot_ref[...] = terms[0]


def merged_bands(dates, bands):
    return min(MERGED, bands - 1) if dates == 4 else 0


def put(res, u, b, i, value):
    whole = value.astype(jnp.int32)
    for jj in range(PAIR):
        res[u, b, jj, i] = whole[jj].astype(jnp.int16)


def finish(fin, tot_ref, coef, score, coef_buf, score_buf, coef_sem, score_sem):
    per, bands = fin.shape[:2]
    copies = []
    tot = tot_ref[...]
    for b in range(bands):
        sigma = jnp.sqrt(tot[:, b:b + 1] / tot[:, bands:bands + 1])
        scale = jnp.broadcast_to(1.0 / sigma, fin.shape[3:])
        for r in range(per):
            cols = slice(r * 128, (r + 1) * 128)
            number = lambda i: fin[r, b, i].astype(jnp.int32).astype(jnp.float32)
            unit = jnp.exp2(number(HARM + 1))
            step = unit * (1.0 / LIMIT)
            for i in range(HARM):
                coef_buf[b, i, :, cols] = number(i) * step
            root = number(HARM) * (1.0 / LIMIT)
            root = root * root
            score_buf[b, :, cols] = root * root * (unit * scale)
        copies.append(pltpu.make_async_copy(coef_buf.at[b], coef.at[b], coef_sem.at[b]))
        copies[-1].start()
    copies.append(pltpu.make_async_copy(score_buf, score, score_sem))
    copies[-1].start()
    for c in copies:
        c.wait()


def local(mesh, stack, quality, days):
    dates, pixes = mesh.shape["date"], mesh.shape["pix"]
    times, bands, rows, width = stack.shape
    block = rows // pixes
    per = pixes // dates
    units = per // PAIR
    total = dates * times
    dims = (dates, pixes, times, bands, block)
    merged = merged_bands(dates, bands)
    notes = max(merged, 1)
    tile = (block, width)
    both = (PAIR,) + tile
    tall = (PAIR * block, width)
    vmem, dma = pltpu.VMEM, pltpu.SemaphoreType.DMA
    f32, bf16 = jnp.float32, jnp.bfloat16
    fin, tot = pl.pallas_call(
        functools.partial(kernel, dims),
        out_shape=(
            vmem((per, bands, HARM + 2) + tile, jnp.int16),
            vmem((1, width), f32),
        ),
        in_specs=[
            pl.BlockSpec(memory_space=pl.ANY),
            pl.BlockSpec(memory_space=pl.ANY),
            pl.BlockSpec(memory_space=pltpu.SMEM),
        ],
        out_specs=(
            pl.BlockSpec(memory_space=pltpu.VMEM),
            pl.BlockSpec(memory_space=pltpu.VMEM),
        ),
        scratch_shapes=[
            vmem((times, 128), f32),
            vmem((times, rows, width), jnp.int32),
            vmem((dates, units, times) + tall, bf16),
            vmem((units, bands + 1, total) + tall, bf16),
            vmem((units, merged + 1, 2 * times) + tall, bf16),
            vmem((dates, times, 128), f32),
            vmem((HARM, total, width), f32),
            vmem((total,) + both, f32),
            vmem((2 * times,) + both, f32),
            vmem((len(PAIR_LIST),) + both, f32),
            vmem((len(PAIR_LIST),) + both, f32),
            vmem((len(PAIR_LIST),) + both, f32),
            vmem(both, f32),
            vmem((units, notes, HARM + 1) + both, f32),
            vmem((units, notes, HARM + 1) + both, f32),
            vmem((units, bands, PAIR, HARM + 2) + tile, jnp.int16),
            vmem((per, bands, HARM + 2) + tile, jnp.int16),
            vmem((bands + 1,) + tile, f32),
            vmem((1, width), f32),
            vmem((dates * pixes, 1, width), f32),
            dma,
            dma((dates,)),
            dma((dates,)),
            dma((units, bands + 1, dates)),
            dma((units, bands + 1, dates)),
            dma((units, merged + 1)),
            dma((units, merged + 1, 2)),
            dma((units,)),
            dma((units, notes)),
            dma((units, notes)),
            dma((units, bands, PAIR)),
            dma((per, bands)),
            dma((per, bands)),
            dma((per, bands)),
            dma((dates, pixes)),
            dma((dates * pixes,)),
        ],
        compiler_params=pltpu.CompilerParams(
            collective_id=0, has_side_effects=True, vmem_limit_bytes=60000000
        ),
    )(stack, quality, days)
    whole = pl.BlockSpec(memory_space=pltpu.VMEM)
    there = pl.BlockSpec(memory_space=pl.ANY)
    coef_shape = (bands, HARM, block, width * per)
    score_shape = (bands, block, width * per)
    return pl.pallas_call(
        finish,
        out_shape=(
            jax.ShapeDtypeStruct(coef_shape, f32),
            jax.ShapeDtypeStruct(score_shape, f32),
        ),
        in_specs=[whole, whole],
        out_specs=(there, there),
        scratch_shapes=[vmem(coef_shape, f32), vmem(score_shape, f32), dma((bands,)), dma],
        compiler_params=pltpu.CompilerParams(vmem_limit_bytes=20000000),
    )(fin, tot)


def solution(mesh):
    return jax.shard_map(
        functools.partial(local, mesh),
        mesh=mesh,
        in_specs=(P("date", None, None, "pix"), P("date", None, "pix"), P("date")),
        out_specs=(P(None, None, "pix", "date"), P(None, "pix", "date")),
        check_vma=False,
    )
```

```python
import functools

import jax
import jax.numpy as jnp
from jax import lax
from jax.experimental import pallas as pl
from jax.experimental.pallas import tpu as pltpu
from jax.sharding import PartitionSpec as P

RIDGE_TERM = 1.0
HARM = 8
PAIR = 2
LAG = 4
DIRECT = 2
MERGED = 6
REST_AT = 5
AHEAD = 1
BEHIND = 4
GRAM_AT = 2
LIMIT = 32767.0
LEVELS = 0x346C

MESH = pl.DeviceIdType.MESH
PAIR_LIST = [(first, second) for first in range(HARM) for second in range(first + 1)]
PAIR_AT = {pair: number for number, pair in enumerate(PAIR_LIST)}


def design_lanes(days):
    rows = [jnp.full((1, 128), day, jnp.int32) for day in days]
    moment_t = jnp.concatenate(rows, 0).astype(jnp.float32)
    lane = lax.broadcasted_iota(jnp.int32, moment_t.shape, 1)
    rate = jnp.where(
        lane < 4, 2.0 * jnp.pi, jnp.where(lane < 6, 4.0 * jnp.pi, 6.0 * jnp.pi))
    phase = rate * moment_t / 365.25
    wave = jnp.where(jnp.bitwise_and(lane, 1) == 0, jnp.cos(phase), jnp.sin(phase))
    linear = (moment_t - 512.0) / 512.0
    return jnp.where(lane == 0, 1.0, jnp.where(lane == 1, linear, wave))


def kernel(dims, stack, quality, days, fin, tot_ref,
           des_in, qbuf, code, raw, side, dall, bdes, wbuf, wside, gbuf, lbuf, lside,
           wsum_ref, note_out, note_in, res, rel, ssum, part, part_all,
           q_sem, des_send, des_recv, raw_send, raw_recv, side_send, side_recv,
           next_send, note_send, note_recv, hop_send, rel_recv, fin_send, fin_recv,
           part_send, part_recv):
    dates, pixes, times, bands, block = dims
    per = pixes // dates
    units = per // PAIR
    tall = PAIR * block
    s = lax.axis_index("date")
    q = lax.axis_index("pix")
    total = dates * times
    place = lax.rem(q, per)
    home = q // per
    merged = merged_bands(dates, bands)
    along = 1 + lax.rem(q, 2)
    across = 3 - along

    def peer_of(k):
        if dates & (dates - 1):
            return lax.rem(s + k, dates)
        return jnp.bitwise_xor(s, k)

    def group(sd):
        flip = lax.rem(q, 2)
        if dates & (dates - 1):
            return lax.rem(home + flip * (dates // 2) + 2 * dates - sd, dates)
        return jnp.bitwise_xor(jnp.bitwise_xor(home, sd), flip * (dates - 1))

    def far_of(r):
        flip = lax.rem(r, 2)
        if dates & (dates - 1):
            return lax.rem(home + s + dates - flip * (dates // 2), dates)
        return jnp.bitwise_xor(jnp.bitwise_xor(home, s), flip * (dates - 1))

    mine = group(s)

    barrier = pltpu.get_barrier_semaphore()
    others = [(k, kk) for k in range(dates) for kk in range(pixes) if k or kk]
    for k, kk in others:
        pl.semaphore_signal(barrier, inc=1, device_id=(peer_of(k), lax.rem(q + kk, pixes)),
                            device_id_type=MESH)

    q_copy = pltpu.make_async_copy(quality, qbuf, q_sem)
    q_copy.start()

    def rows_of(g, u):
        first = (g * units + u) * tall
        return pl.ds(pl.multiple_of(first, tall), tall)

    def mine_at(sd):
        return pl.ds(pl.multiple_of(sd * times, times), times)

    for u in range(units):
        for b in range(bands):
            pltpu.make_async_copy(
                stack.at[:, b, rows_of(mine, u), :], raw.at[u, b, mine_at(s)],
                raw_recv.at[u, b, s]).start()
            if b < merged:
                pltpu.make_async_copy(
                    stack.at[:, b, rows_of(group(peer_of(along)), u), :],
                    side.at[u, b, pl.ds(0, times)], side_recv.at[u, b, 0]).start()

    des_in[...] = design_lanes([days[r] for r in range(times)])
    q_copy.wait()
    for g in range(dates):
        for u in range(units):
            first = (g * units + u) * tall
            bits = qbuf[:, first:first + tall, :]
            digit = jnp.bitwise_and(jnp.right_shift(bits, 6), 12)
            value = jnp.bitwise_and(jnp.right_shift(jnp.full_like(bits, LEVELS), digit), 15)
            value = jnp.where(jnp.bitwise_and(bits, 8) == 0, value, 0)
            code[g, u] = value.astype(jnp.float32).astype(jnp.bfloat16)

    pl.semaphore_wait(barrier, len(others))

    def des_copy(k):
        return pltpu.make_async_remote_copy(
            des_in, dall.at[s], des_send.at[k], des_recv.at[s],
            device_id=(peer_of(k), q), device_id_type=MESH)

    def values_of(u, b, k):
        return stack.at[:, b, rows_of(group(peer_of(k)), u), :]

    def codes_of(u, k):
        return code.at[group(peer_of(k)), u]

    def raw_copy(src, u, b, k, slot):
        return pltpu.make_async_remote_copy(
            src, raw.at[u, b, mine_at(s)], raw_send.at[u, b, slot], raw_recv.at[u, b, s],
            device_id=(peer_of(k), q), device_id_type=MESH)

    def side_copy(src, u, b):
        return pltpu.make_async_remote_copy(
            src, side.at[u, b, pl.ds(times, times)], side_send.at[u, b], side_recv.at[u, b, 1],
            device_id=(peer_of(across), q), device_id_type=MESH)

    def next_copy(u):
        first = peer_of(across)
        return pltpu.make_async_remote_copy(
            side.at[u, merged, pl.ds(times, times)], raw.at[u, bands, mine_at(first)],
            next_send.at[u], raw_recv.at[u, bands, first],
            device_id=(peer_of(along), q), device_id_type=MESH)

    def note_copy(u, b):
        return pltpu.make_async_remote_copy(
            note_out.at[u, b], note_in.at[u, b], note_send.at[u, b], note_recv.at[u, b],
            device_id=(peer_of(along), q), device_id_type=MESH)

    order = list(range(dates - 1, 0, -1))

    def code_copies(u):
        if not merged:
            return [raw_copy(codes_of(u, k), u, bands, k, k) for k in order]
        return [side_copy(codes_of(u, dates - 1), u, merged),
                raw_copy(codes_of(u, across), u, bands, across, 1),
                raw_copy(codes_of(u, along), u, bands, along, 2)]

    def merged_copies(u, b):
        return [lambda: side_copy(values_of(u, b, dates - 1), u, b),
                lambda: raw_copy(values_of(u, b, across), u, b, across, 1)]

    def rest_copies(u, b):
        return [raw_copy(values_of(u, b, k), u, b, k, k) for k in order]

    for k in order:
        des_copy(k).start()
    for u in range(units):
        for c in code_copies(u):
            c.start()
        for b in range(merged + AHEAD):
            if b < merged:
                merged_copies(u, b)[0]().start()
            if b >= AHEAD:
                merged_copies(u, b - AHEAD)[1]().start()
        if not merged:
            for b in range(bands):
                for c in rest_copies(u, b):
                    c.start()
    for u in range(units):
        pltpu.make_async_copy(
            code.at[mine, u], raw.at[u, bands, mine_at(s)],
            raw_recv.at[u, bands, s]).start()
        if merged:
            pltpu.make_async_copy(
                code.at[group(peer_of(along)), u], side.at[u, merged, pl.ds(0, times)],
                side_recv.at[u, merged, 0]).start()

    def raw_wait(u, b, sd):
        there = raw.at[u, b, mine_at(sd)]
        pltpu.make_async_copy(there, there, raw_recv.at[u, b, sd]).wait()

    dall[s] = des_in[...]

    zero = jnp.zeros((PAIR, block, 128), jnp.float32)
    zero_one = jnp.zeros((block, 128), jnp.float32)
    for b in range(bands + 1):
        ssum[b] = zero_one

    def side_wait(u, b, slot):
        there = side.at[u, b, pl.ds(pl.multiple_of(slot * times, times), times)]
        pltpu.make_async_copy(there, there, side_recv.at[u, b, slot]).wait()

    def spread(k, wait):
        sd = peer_of(k)
        if wait:
            pltpu.make_async_copy(dall.at[sd], dall.at[sd], des_recv.at[sd]).wait()

        rows = dall[sd]
        for i in range(HARM):
            bdes[i, mine_at(sd), :] = jnp.broadcast_to(rows[:, i:i + 1], rows.shape)

    def design(t, i):
        return jnp.broadcast_to(bdes[i, pl.ds(t, 1), :], (block, 128))

    def pair_of(value):
        return value.astype(jnp.float32).reshape(PAIR, block, 128)

    def by_source(count, source_of, wait, body, carry, unroll):
        def source(n, carry):
            sd = source_of(n)
            wait(n, sd)
            return lax.fori_loop(
                0, times, lambda r, c: body(sd * times + r, n * times + r, c), carry,
                unroll=unroll)

        return lax.fori_loop(0, count, source, carry)

    every = (dates, peer_of)
    near = (2, lambda n: peer_of(n * across)) if merged else every
    far = (2, lambda n: peer_of(along + n * (dates - 1 - along)))

    def gram_over(sources, wait, code_at, weight_at, weight_to, out):
        def body(jj):
            def step(t, place_t, carry):
                if jj == 0:
                    both = pair_of(code_at(t, place_t)) * (1.0 / 12.0)
                    weight_to(t, place_t, both)
                    w = both[0]
                else:
                    w = weight_at(t, place_t, jj)
                d = [design(t, i) for i in range(HARM)]
                wd = [w] + [w * d[i] for i in range(1, HARM)]
                return tuple(
                    carry[n] + (wd[first] if second == 0 else wd[first] * d[second])
                    for n, (first, second) in enumerate(PAIR_LIST))
            return step

        start = (zero_one,) * len(PAIR_LIST)
        for jj in range(PAIR):
            gram = by_source(
                *sources, wait if jj == 0 else lambda n, sd: None, body(jj), start, 2)
            for n in range(len(PAIR_LIST)):
                out[n, jj] = gram[n]

    def factor(gram, out):
        lower = {}
        for first in range(HARM):
            for second in range(first + 1):
                value = gram[PAIR_AT[first, second]]
                if first == second:
                    value = value + RIDGE_TERM
                for inner in range(second):
                    value = value - lower[first, inner] * lower[second, inner]
                if first == second:
                    lower[first, first] = lax.rsqrt(value)
                else:
                    lower[first, second] = value * lower[second, second]
                out[PAIR_AT[first, second]] = lower[first, second]

    def solve(moment, lref):
        low = lambda first, second: lref[PAIR_AT[first, second]]
        forward = []
        for first in range(HARM):
            value = moment[first]
            for inner in range(first):
                value = value - low(first, inner) * forward[inner]
            forward.append(value * low(first, first))
        back = [None] * HARM
        for first in range(HARM - 1, -1, -1):
            value = forward[first]
            for inner in range(HARM - 1, first, -1):
                value = value - low(inner, first) * back[inner]
            back[first] = value * low(first, first)
        return back

    def moment_over(sources, wait, value_at, weight_at):
        def body(t, place_t, carry):
            wy = weight_at(t, place_t) * pair_of(value_at(t, place_t))
            return tuple(
                carry[i] + (wy if i == 0 else design(t, i) * wy) for i in range(HARM))

        return by_source(*sources, wait, body, (zero,) * HARM, 8)

    def residual_over(sources, back, value_at, weight_at):
        def body(t, place_t, ssr):
            terms = [back[0]] + [design(t, i) * back[i] for i in range(1, HARM)]
            while len(terms) > 1:
                terms = [terms[i] + terms[i + 1] for i in range(0, len(terms), 2)]
            diff = pair_of(value_at(t, place_t)) - terms[0]
            return ssr + weight_at(t, place_t) * diff * diff

        return by_source(*sources, lambda n, sd: None, body, zero, 8)

    def side_gram(u):
        def wait(n, sd):
            side_wait(u, merged, n)

            @pl.when(n == 1)
            def _():
                next_copy(u).start()

        def keep(t, place_t, both):
            wside[place_t] = both

        gram_over(near, wait, lambda t, place_t: side[u, merged, place_t],
                  lambda t, place_t, jj: wside[place_t, jj], keep, lside)
        factor([lside[n] for n in range(len(PAIR_LIST))], lside)

    def side_step(u, b):
        value_at = lambda t, place_t: side[u, b, place_t]
        weight_at = lambda t, place_t: wside[place_t]
        moment = moment_over(near, lambda n, sd: side_wait(u, b, n), value_at, weight_at)
        back = solve(moment, lside)
        for i in range(HARM):
            note_out[u, b, i] = back[i]
        note_out[u, b, HARM] = residual_over(near, back, value_at, weight_at)
        note_copy(u, b).start()

    def own_gram(u):
        def keep(t, place_t, both):
            wbuf[t] = both

        def over(sources, out):
            gram_over(sources, lambda n, sd: raw_wait(u, bands, sd),
                      lambda t, place_t: raw[u, bands, t],
                      lambda t, place_t, jj: wbuf[t, jj], keep, out)

        over(near, lbuf)
        if merged:
            over(far, gbuf)
            gram = [lbuf[n] + gbuf[n] for n in range(len(PAIR_LIST))]
        else:
            gram = [lbuf[n] for n in range(len(PAIR_LIST))]
        wsum_ref[...] = 1.0 / (gram[0] + 1.0)
        ssum[bands] = ssum[bands] + jnp.sum(gram[0], 0)
        factor(gram, lbuf)

    def far_gram_times(vector):
        rows = []
        for first in range(HARM):
            row = None
            for second in range(HARM):
                pair = (max(first, second), min(first, second))
                term = gbuf[PAIR_AT[pair]] * vector[second]
                row = term if row is None else row + term
            rows.append(row)
        return rows

    def hop(u, b, start):
        for jj in range(PAIR):
            p = mine * per + PAIR * u + jj

            def act(dst, sem):
                @pl.when(p != q)
                def _():
                    c = pltpu.make_async_remote_copy(
                        res.at[u, b, jj], dst, hop_send.at[u, b, jj], sem,
                        device_id=(s, p), device_id_type=MESH)
                    c.start() if start else c.wait_send()

                if start:
                    @pl.when(p == q)
                    def _():
                        pltpu.make_async_copy(res.at[u, b, jj], dst, sem).start()

            @pl.when(home == s)
            def _():
                act(fin.at[place, b], fin_recv.at[place, b])

            late = u * bands + b >= units * bands - DIRECT

            @pl.when(jnp.logical_and(home != s, jnp.logical_not(late)))
            def _():
                act(rel.at[place, b], rel_recv.at[place, b])

            @pl.when(jnp.logical_and(home != s, late))
            def _():
                c = pltpu.make_async_remote_copy(
                    res.at[u, b, jj], fin.at[place, b], hop_send.at[u, b, jj],
                    fin_recv.at[place, b], device_id=(home, p), device_id_type=MESH)
                c.start() if start else c.wait_send()

    def band_step(u, b, with_note):
        value_at = lambda t, place_t: raw[u, b, t]
        weight_at = lambda t, place_t: wbuf[t]
        sources = near if with_note else every
        moment = moment_over(
            sources, lambda n, sd: raw_wait(u, b, sd), value_at, weight_at)
        if with_note:
            pltpu.make_async_copy(note_in.at[u, b], note_in.at[u, b], note_recv.at[u, b]).wait()
            fit = [note_in[u, b, i] for i in range(HARM)]
            rows = far_gram_times(fit)
            moment = [moment[i] + (rows[i] + fit[i]) for i in range(HARM)]
        back = solve(moment, lbuf)
        ssr = residual_over(sources, back, value_at, weight_at)
        if with_note:
            fit = [note_in[u, b, i] for i in range(HARM)]
            shift = [back[i] - fit[i] for i in range(HARM)]
            rows = far_gram_times(shift)
            extra = note_in[u, b, HARM]
            for i in range(HARM):
                extra = extra + shift[i] * (rows[i] - 2.0 * fit[i])
            ssr = jnp.maximum(ssr + extra, 0.0)
        ratio = jnp.sqrt(ssr * wsum_ref[...])
        peak = ratio
        for i in range(HARM):
            peak = jnp.maximum(peak, jnp.abs(back[i]))
        level = jnp.ceil(jnp.log2(jnp.maximum(peak, 1e-36)) + 0.01)
        inverse = jnp.exp2(-level)
        scale = inverse * LIMIT
        for i in range(HARM):
            put(res, u, b, i, jnp.floor(jnp.clip(back[i] * scale, -LIMIT, LIMIT) + 0.5))
        root = jnp.sqrt(jnp.sqrt(jnp.minimum(ratio * inverse, 1.0)))
        put(res, u, b, HARM, jnp.floor(root * LIMIT + 0.5))
        put(res, u, b, HARM + 1, level)
        ssum[b] = ssum[b] + jnp.sum(ssr, 0)
        hop(u, b, True)

    def pass_on(r, b, start):
        far = far_of(r)

        @pl.when(far != s)
        def _():
            c = pltpu.make_async_remote_copy(
                rel.at[r, b], fin.at[r, b], fin_send.at[r, b], fin_recv.at[r, b],
                device_id=(far, q), device_id_type=MESH)
            if start:
                pltpu.make_async_copy(rel.at[r, b], rel.at[r, b], rel_recv.at[r, b]).wait()
                c.start()
            else:
                c.wait_send()

    def relay(n):
        b = lax.rem(n, bands)

        @pl.when(n // bands == place // PAIR)
        def _():
            for r in range(per):
                pass_on(r, b, True)

    def rest_at(u, act):
        for b in range(merged, bands):
            for c in rest_copies(u, b):
                act(c)

    if merged:
        spread(0, False)
        spread(across, True)
    else:
        for k in range(dates):
            spread(k, k > 0)

    behind = BEHIND if merged else 1
    gram_at = GRAM_AT if merged else 0
    steps = bands + behind

    @pl.loop(0, units * steps)
    def _(n):
        u = n // steps
        step = lax.rem(n, steps)
        if merged:
            @pl.when(step == 0)
            def _():
                side_gram(u)

            @pl.when(step < merged)
            def _():
                side_step(u, step)

            @pl.when(n == 0)
            def _():
                spread(along, True)
                spread(dates - 1, True)

            @pl.when(step == REST_AT)
            def _():
                rest_at(u, lambda c: c.start())

        @pl.when(step == gram_at)
        def _():
            own_gram(u)

        b = step - behind
        if merged:
            @pl.when(jnp.logical_and(b >= 0, b < merged))
            def _():
                band_step(u, b, True)

        if merged < bands:
            @pl.when(b >= merged)
            def _():
                band_step(u, b, False)

        done = u * bands + b

        @pl.when(jnp.logical_and(b >= 0, done >= LAG))
        def _():
            relay(done - LAG)

    sums = jnp.concatenate(
        [jnp.sum(ssum[b], 0, keepdims=True) for b in range(bands + 1)], 0)
    sums = jnp.broadcast_to(jnp.sum(sums, 1, keepdims=True), sums.shape)
    lane = lax.broadcasted_iota(jnp.int32, sums.shape, 1)
    row = lax.broadcasted_iota(jnp.int32, sums.shape, 0)
    part[...] = jnp.sum(jnp.where(lane == row, sums, 0.0), 0, keepdims=True)
    here = s * pixes + q

    def part_copy(k, kk):
        return pltpu.make_async_remote_copy(
            part, part_all.at[here], part_send.at[k, kk], part_recv.at[here],
            device_id=(peer_of(k), lax.rem(q + kk, pixes)), device_id_type=MESH)

    for k, kk in reversed(others):
        part_copy(k, kk).start()
    part_all[here] = part[...]
    for n in range(LAG, DIRECT, -1):
        relay(units * bands - n)

    for k in range(1, dates):
        des_copy(k).wait_send()
    for k, kk in others:
        part_copy(k, kk).wait_send()

    @pl.loop(0, units)
    def _(u):
        for c in code_copies(u):
            c.wait_send()
        if merged:
            next_copy(u).wait_send()

            @pl.loop(0, merged)
            def _(b):
                for c in merged_copies(u, b):
                    c().wait_send()
                note_copy(u, b).wait_send()
            rest_at(u, lambda c: c.wait_send())
        else:
            @pl.loop(0, bands)
            def _(b):
                for c in rest_copies(u, b):
                    c.wait_send()

        @pl.loop(0, bands)
        def _(b):
            hop(u, b, False)

    @pl.loop(0, bands)
    def _(b):
        @pl.when((place // PAIR) * bands + b < units * bands - DIRECT)
        def _():
            for r in range(per):
                pass_on(r, b, False)

    @pl.loop(0, bands)
    def _(b):
        for r in range(per):
            pltpu.make_async_copy(fin.at[r, b], fin.at[r, b], fin_recv.at[r, b]).wait()

    for k, kk in others:
        there = peer_of(k) * pixes + lax.rem(q + kk, pixes)
        pltpu.make_async_copy(part_all.at[there], part_all.at[there], part_recv.at[there]).wait()
    terms = [part_all[n] for n in range(dates * pixes)]
    while len(terms) > 1:
        terms = [sum(terms[i:i + 2]) for i in range(0, len(terms), 2)]
    tot_ref[...] = terms[0]


def merged_bands(dates, bands):
    return min(MERGED, bands - 1) if dates == 4 else 0


def put(res, u, b, i, value):
    whole = value.astype(jnp.int32)
    for jj in range(PAIR):
        res[u, b, jj, i] = whole[jj].astype(jnp.int16)


def finish(fin, tot_ref, coef, score, coef_buf, score_buf, coef_sem, score_sem):
    per, bands = fin.shape[:2]
    copies = []
    tot = tot_ref[...]
    for b in range(bands):
        sigma = jnp.sqrt(tot[:, b:b + 1] / tot[:, bands:bands + 1])
        scale = jnp.broadcast_to(1.0 / sigma, fin.shape[3:])
        for r in range(per):
            cols = slice(r * 128, (r + 1) * 128)
            number = lambda i: fin[r, b, i].astype(jnp.int32).astype(jnp.float32)
            unit = jnp.exp2(number(HARM + 1))
            step = unit * (1.0 / LIMIT)
            for i in range(HARM):
                coef_buf[b, i, :, cols] = number(i) * step
            root = number(HARM) * (1.0 / LIMIT)
            root = root * root
            score_buf[b, :, cols] = root * root * (unit * scale)
        copies.append(pltpu.make_async_copy(coef_buf.at[b], coef.at[b], coef_sem.at[b]))
        copies[-1].start()
    copies.append(pltpu.make_async_copy(score_buf, score, score_sem))
    copies[-1].start()
    for c in copies:
        c.wait()


def local(mesh, stack, quality, days):
    dates, pixes = mesh.shape["date"], mesh.shape["pix"]
    times, bands, rows, width = stack.shape
    block = rows // pixes
    per = pixes // dates
    units = per // PAIR
    total = dates * times
    dims = (dates, pixes, times, bands, block)
    merged = merged_bands(dates, bands)
    notes = max(merged, 1)
    tile = (block, width)
    both = (PAIR,) + tile
    tall = (PAIR * block, width)
    vmem, dma = pltpu.VMEM, pltpu.SemaphoreType.DMA
    f32, bf16 = jnp.float32, jnp.bfloat16
    fin, tot = pl.pallas_call(
        functools.partial(kernel, dims),
        out_shape=(
            vmem((per, bands, HARM + 2) + tile, jnp.int16),
            vmem((1, width), f32),
        ),
        in_specs=[
            pl.BlockSpec(memory_space=pl.ANY),
            pl.BlockSpec(memory_space=pl.ANY),
            pl.BlockSpec(memory_space=pltpu.SMEM),
        ],
        out_specs=(
            pl.BlockSpec(memory_space=pltpu.VMEM),
            pl.BlockSpec(memory_space=pltpu.VMEM),
        ),
        scratch_shapes=[
            vmem((times, 128), f32),
            vmem((times, rows, width), jnp.int32),
            vmem((dates, units, times) + tall, bf16),
            vmem((units, bands + 1, total) + tall, bf16),
            vmem((units, merged + 1, 2 * times) + tall, bf16),
            vmem((dates, times, 128), f32),
            vmem((HARM, total, width), f32),
            vmem((total,) + both, f32),
            vmem((2 * times,) + both, f32),
            vmem((len(PAIR_LIST),) + both, f32),
            vmem((len(PAIR_LIST),) + both, f32),
            vmem((len(PAIR_LIST),) + both, f32),
            vmem(both, f32),
            vmem((units, notes, HARM + 1) + both, f32),
            vmem((units, notes, HARM + 1) + both, f32),
            vmem((units, bands, PAIR, HARM + 2) + tile, jnp.int16),
            vmem((per, bands, HARM + 2) + tile, jnp.int16),
            vmem((bands + 1,) + tile, f32),
            vmem((1, width), f32),
            vmem((dates * pixes, 1, width), f32),
            dma,
            dma((dates,)),
            dma((dates,)),
            dma((units, bands + 1, dates)),
            dma((units, bands + 1, dates)),
            dma((units, merged + 1)),
            dma((units, merged + 1, 2)),
            dma((units,)),
            dma((units, notes)),
            dma((units, notes)),
            dma((units, bands, PAIR)),
            dma((per, bands)),
            dma((per, bands)),
            dma((per, bands)),
            dma((dates, pixes)),
            dma((dates * pixes,)),
        ],
        compiler_params=pltpu.CompilerParams(
            collective_id=0, has_side_effects=True, vmem_limit_bytes=60000000
        ),
    )(stack, quality, days)
    whole = pl.BlockSpec(memory_space=pltpu.VMEM)
    there = pl.BlockSpec(memory_space=pl.ANY)
    coef_shape = (bands, HARM, block, width * per)
    score_shape = (bands, block, width * per)
    return pl.pallas_call(
        finish,
        out_shape=(
            jax.ShapeDtypeStruct(coef_shape, f32),
            jax.ShapeDtypeStruct(score_shape, f32),
        ),
        in_specs=[whole, whole],
        out_specs=(there, there),
        scratch_shapes=[vmem(coef_shape, f32), vmem(score_shape, f32), dma((bands,)), dma],
        compiler_params=pltpu.CompilerParams(vmem_limit_bytes=20000000),
    )(fin, tot)


def solution(mesh):
    return jax.shard_map(
        functools.partial(local, mesh),
        mesh=mesh,
        in_specs=(P("date", None, None, "pix"), P("date", None, "pix"), P("date")),
        out_specs=(P(None, None, "pix", "date"), P(None, "pix", "date")),
        check_vma=False,
    )
```
